8 devices in a mesh: sys: 1 (over z), zdom: 2 (over y), ydom: 4 (over x, core).
Axes of the slice: x: 2, y: 2, z: 1, core: 2. Of those that a mesh axis runs over, the one named last changes fastest.
Arguments:
- charge: float32 [131072], P(('sys', 'ydom', 'zdom'))
- real_mask: int32 [131072], P(('sys', 'ydom', 'zdom'))
- grid_idx: int32 [131072, 3], P(('sys', 'ydom', 'zdom'))
- spline_w: float32 [131072, 3, 4], P(('sys', 'ydom', 'zdom'))
- influence: float32 [96, 96, 96], P(('sys', 'ydom'), 'zdom')
Outputs:
- output 1: float32 [96, 96, 96], P(('sys', 'ydom'), 'zdom')
- output 2: float32 [1], P('sys')
All inputs are finite; a program needn't handle non-finite values.
Results may differ from the reference program's by a relative error of at most 0.001.
Values are sent between devices in bfloat16 or wider.
A program may use at most 1 GiB of HBM per device.

```python
import jax
import jax.numpy as jnp
from jax import lax

GRID_SIDE = 96
PER_DEV = 16384
Y_DEVS = 4
Z_DEVS = 2


def bspline_weights(frac_part):
    frac_sq = frac_part * frac_part
    frac_cube = frac_sq * frac_part
    w_zero = (1.0 - frac_part) * (1.0 - frac_part) * (1.0 - frac_part) / 6.0
    w_one = (3.0 * frac_cube - 6.0 * frac_sq + 4.0) / 6.0
    w_two = (-3.0 * frac_cube + 3.0 * frac_sq + 3.0 * frac_part + 1.0) / 6.0
    w_three = frac_cube / 6.0
    return jnp.stack([w_zero, w_one, w_two, w_three], axis=-1)


def edge_index(key, count, length):
    key_near, key_edge, key_any = jax.random.split(key, 3)
    near_edge = jax.random.randint(key_near, (count,), 0, 2)
    at_edge = length - 3 + jax.random.randint(key_edge, (count,), 0, 3)
    anywhere = jax.random.randint(key_any, (count,), 0, length)
    return jnp.where(near_edge == 1, at_edge, anywhere)


def setup_inputs(seed: int = 0, part: int = 0) -> dict:
    dev_count = Y_DEVS * Z_DEVS
    slot_count = dev_count * PER_DEV
    len_y = GRID_SIDE // Y_DEVS
    len_z = GRID_SIDE // Z_DEVS
    sub_keys = jax.random.split(jax.random.fold_in(jax.random.key(seed), part), 8)
    real_count = jax.random.randint(sub_keys[0], (dev_count, 1), PER_DEV // 8, PER_DEV + 1)
    slot_rank = jax.random.randint(sub_keys[1], (dev_count, PER_DEV), 0, PER_DEV)
    real_mask = (slot_rank < real_count).astype(jnp.int32).reshape(slot_count)
    x_idx = jax.random.randint(sub_keys[2], (slot_count,), 0, GRID_SIDE)
    y_idx = edge_index(sub_keys[3], slot_count, len_y)
    z_idx = edge_index(sub_keys[4], slot_count, len_z)
    grid_idx = jnp.stack([x_idx, y_idx, z_idx], axis=1).astype(jnp.int32)
    charge = jax.random.normal(sub_keys[5], (slot_count,), jnp.float32)
    frac_part = jax.random.uniform(sub_keys[6], (slot_count, 3), jnp.float32)
    spline_w = bspline_weights(frac_part).astype(jnp.float32)
    influence = jax.random.uniform(sub_keys[7], (GRID_SIDE, GRID_SIDE, GRID_SIDE), jnp.float32, 0.5, 1.5) * (20.0 / slot_count)
    return {'charge': charge, 'real_mask': real_mask, 'grid_idx': grid_idx, 'spline_w': spline_w, 'influence': influence}


def reference(charge, real_mask, grid_idx, spline_w, influence):
    slot_count = Y_DEVS * Z_DEVS * PER_DEV
    len_y = GRID_SIDE // Y_DEVS
    len_z = GRID_SIDE // Z_DEVS
    device = jnp.arange(slot_count) // PER_DEV
    base_x = grid_idx[:, 0]
    base_y = grid_idx[:, 1] + (device // Z_DEVS) * len_y
    base_z = grid_idx[:, 2] + (device % Z_DEVS) * len_z
    weight = charge * real_mask.astype(charge.dtype)

    def add_tap(flat_grid, tap_id):
        off_x = tap_id // 16
        off_y = (tap_id // 4) % 4
        off_z = tap_id % 4
        pos_x = (base_x + off_x) % GRID_SIDE
        pos_y = (base_y + off_y) % GRID_SIDE
        pos_z = (base_z + off_z) % GRID_SIDE
        tap_value = weight * spline_w[:, 0, off_x] * spline_w[:, 1, off_y] * spline_w[:, 2, off_z]
        flat_idx = (pos_x * GRID_SIDE + pos_y) * GRID_SIDE + pos_z
        return flat_grid.at[flat_idx].add(tap_value), None

    flat_grid = lax.scan(add_tap, jnp.zeros((GRID_SIDE * GRID_SIDE * GRID_SIDE,), charge.dtype), jnp.arange(64))[0]
    charge_grid = flat_grid.reshape(GRID_SIDE, GRID_SIDE, GRID_SIDE)
    spectrum = jnp.fft.fftn(charge_grid)
    mode_energy = 0.5 * influence * (spectrum.real * spectrum.real + spectrum.imag * spectrum.imag)
    energy = jnp.sum(mode_energy) / (GRID_SIDE * GRID_SIDE * GRID_SIDE)
    return mode_energy, jnp.reshape(energy, (1,))
```

```python
import functools
import math
import jax
import jax.numpy as jnp
import numpy as np
from jax import lax
from jax.experimental import pallas as pl
from jax.experimental.pallas import tpu as pltpu
from jax.sharding import PartitionSpec as P

MESH = pl.DeviceIdType.MESH
F32 = jnp.float32
BF16 = jnp.bfloat16
G = 96
Y_DEVS = 4
Z_DEVS = 2
LEN_Y = 24
LEN_Z = 48
KX = 24
KY = 48
STEP = 512
GHOST_CHUNK = 2
ROWS = (368, 368, 368, 336)
GHOST_ROW = (320, 320, 320, 288)
WIDTH = (384, 384, 512, 384)
BLOCKS = (12, 12, 15, 12)
Z_SLOT = (0, 12, 36, 24)
Z_SLOTS = 52


def split_np(values):
    high = np.asarray(values, np.float32).astype(jnp.bfloat16)
    low = (np.asarray(values, np.float64) - high.astype(np.float64)).astype(jnp.bfloat16)
    return high, low


def dft_x():
    table = np.zeros((Y_DEVS, 2, KX, 128))
    for dest in range(Y_DEVS):
        angle = 2 * math.pi * (np.outer(np.arange(KX) + KX * dest, np.arange(G)) % G) / G
        table[dest, 0, :, :G] = np.cos(angle)
        table[dest, 1, :, :G] = -np.sin(angle)
    high, low = split_np(table.reshape(Y_DEVS * 2 * KX, 128))
    return np.concatenate([high, high], axis=1), low


def dft_y():
    table = np.zeros((2, Y_DEVS, 32, Z_DEVS, 128))
    for source in range(Y_DEVS):
        y_pos = LEN_Y * source + np.arange(LEN_Y + 3)
        for dest in range(Z_DEVS):
            angle = 2 * math.pi * (np.outer(y_pos, np.arange(KY) + KY * dest) % G) / G
            table[0, source, :LEN_Y + 3, dest, :KY] = np.cos(angle)
            table[1, source, :LEN_Y + 3, dest, :KY] = np.sin(angle)
            table[0, source, :LEN_Y + 3, dest, KY:2 * KY] = -np.sin(angle)
            table[1, source, :LEN_Y + 3, dest, KY:2 * KY] = np.cos(angle)
    return split_np(table.reshape(2 * Y_DEVS * 32, Z_DEVS * 128))


def dft_z():
    table = np.zeros((Z_DEVS, Z_SLOTS, 2, 128))
    for source in range(Z_DEVS):
        for chunk in range(4):
            for block in range(BLOCKS[chunk]):
                z_pos = LEN_Z * source + (4 * block + chunk if block < 12 else LEN_Z + block - 12)
                angle = 2 * math.pi * ((z_pos * np.arange(G)) % G) / G
                table[source, Z_SLOT[chunk] + block, 0, :G] = np.cos(angle)
                table[source, Z_SLOT[chunk] + block, 1, :G] = np.sin(angle)
    return split_np(table.reshape(Z_DEVS * Z_SLOTS, 256))


def split(values):
    high = values.astype(BF16)
    return high, (values - high.astype(F32)).astype(BF16)


def dot(lhs, rhs, lhs_dim, rhs_dim):
    return lax.dot_general(lhs, rhs, (((lhs_dim,), (rhs_dim,)), ((), ())), preferred_element_type=F32)


def kernel(charge, mask, grid_idx, spline_w, influence, fx2, fx_low, fy_high, fy_low, fz_high, fz_low,
           mode_out, energy_out,
           line_x, line_y, tap_z, lhs_a, lhs_b, rhs_a, rhs_b, total, packed, ghosts,
           send0, send1, send2, send3, recv0, recv1, recv2, recv3, half0, half1, half2, half3, zbuf, part, parts,
           y_send_sem, y_recv_sem, z_send_sem, z_recv_sem, e_send_sem, e_recv_sem):
    slots = charge.shape[1]
    me_y = lax.axis_index('ydom')
    me_z = lax.axis_index('zdom')
    me = me_z * Y_DEVS + me_y
    sends, recvs, halves = (send0, send1, send2, send3), (recv0, recv1, recv2, recv3), (half0, half1, half2, half3)

    def device(rank):
        return {'zdom': rank // Y_DEVS, 'ydom': rank % Y_DEVS}

    barrier = pltpu.get_barrier_semaphore()
    for shift in range(1, 8):
        pl.semaphore_signal(barrier, inc=1, device_id=device((me + shift) % 8), device_id_type=MESH)

    row16 = lax.broadcasted_iota(jnp.int32, (16, STEP), 0)
    row96 = lax.broadcasted_iota(jnp.int32, (G, STEP), 0)
    patterns = (row16, jnp.where(row16 < 8, row16 + 16, row16 - 8), row16 + 8, row16 % 4 + 24,
                jnp.where(row16 < 8, row16 + 16, jnp.where(row16 < 12, row16 + 16, 99)))

    def prepare(start):
        at = pl.ds(start, STEP)
        base_x, base_y, base_z = grid_idx[0:1, at], grid_idx[1:2, at], grid_idx[2:3, at]
        weight = charge[0:1, at] * mask[0:1, at].astype(F32)
        values = jnp.zeros((G, STEP), F32)
        for tap in range(4):
            pos = base_x + tap
            pos = jnp.where(pos >= G, pos - G, pos)
            values = jnp.where(row96 == pos, spline_w[0, tap:tap + 1, at] * weight, values)
        line_x[:, at] = values
        for index, pattern in enumerate(patterns):
            values = jnp.zeros((16, STEP), F32)
            offset = pattern - base_y
            for tap in range(4):
                values = jnp.where(offset == tap, spline_w[1, tap:tap + 1, at], values)
            high, low = split(values)
            line_y[index, 0, :, at] = high
            line_y[index, 1, :, at] = low
        for chunk in range(4):
            tap = (chunk - base_z) & 3
            values = jnp.where(tap < 2, jnp.where(tap == 0, spline_w[2, 0:1, at], spline_w[2, 1:2, at]),
                               jnp.where(tap == 2, spline_w[2, 2:3, at], spline_w[2, 3:4, at]))
            tap_z[chunk:chunk + 1, at] = values
            tap_z[4 + chunk:5 + chunk, at] = ((base_z + tap) >> 2).astype(F32)

    def build(chunk, start, lhs, rhs):
        at = pl.ds(start, STEP)
        high, low = split(line_x[:, at] * tap_z[chunk:chunk + 1, at])
        rhs[0:G, :] = high
        rhs[128:128 + G, :] = low
        block = jnp.broadcast_to(tap_z[4 + chunk:5 + chunk, at], (16, STEP))
        block_a = block.astype(BF16)
        block_b = (block - (row16 // 8).astype(F32)).astype(BF16)
        block_g = (block - (row16 // 4).astype(F32)).astype(BF16)
        tiles = []
        for pair in range(6):
            tiles += [(block_a, 2 * pair, 0), (block_b, 2 * pair, 1), (block_a, 2 * pair + 1, 2)]
        if chunk < 3:
            tiles += [(block_a, 12, 0), (block_a, 12, 4)]
        tiles += [(block_g, 0, 3), (block_g, 4, 3), (block_g, 8, 3)]
        zero = jnp.zeros((16, STEP), BF16)
        for index, (source, value, pattern) in enumerate(tiles):
            hit = source == jnp.asarray(value, BF16)
            for half in range(2):
                lhs[half * ROWS[chunk] + 16 * index:half * ROWS[chunk] + 16 * index + 16, :] = jnp.where(
                    hit, line_y[pattern, half, :, at], zero)

    def spread(chunk):
        rows = ROWS[chunk]

        def fill(step, lhs, rhs):
            start = pl.multiple_of(jnp.minimum(step, slots // STEP - 1) * STEP, STEP)
            if chunk == 0:
                prepare(start)
            build(chunk, start, lhs, rhs)

        def add(lhs, rhs):
            product = dot(lhs[0:2 * rows, :], rhs[...], 1, 1)
            total[0:rows, :] += product[:rows] + product[rows:]

        total[...] = jnp.zeros_like(total)
        fill(0, lhs_a, rhs_a)

        def body(pair, carry):
            add(lhs_a, rhs_a)
            fill(2 * pair + 1, lhs_b, rhs_b)
            add(lhs_b, rhs_b)
            fill(2 * pair + 2, lhs_a, rhs_a)
            return carry

        lax.fori_loop(0, slots // STEP // 2, body, 0)

    def transform_x(chunk):
        row8 = lax.broadcasted_iota(jnp.int32, (8, 128), 0)

        def lines(start, count):
            return total[start:start + count, 0:128] + total[start:start + count, 128:256]

        for pair in range(6):
            ghost = lines(GHOST_ROW[chunk] + 8 * pair, 8)
            packed[64 * pair:64 * pair + 24, :] = lines(48 * pair, 24)
            packed[64 * pair + 24:64 * pair + 32, :] = jnp.where(row8 < 4, ghost, 0.0)
            packed[64 * pair + 32:64 * pair + 56, :] = lines(48 * pair + 24, 24)
            packed[64 * pair + 56:64 * pair + 64, :] = jnp.where(row8 < 4, pltpu.roll(ghost, 4, 0), 0.0)
        if chunk < 3:
            ghosts[32 * chunk:32 * chunk + 32, :] = lines(288, 32)
        values = packed[...]
        if chunk == GHOST_CHUNK:
            values = jnp.concatenate([values, ghosts[...]], axis=0)
        high, low = split(values)
        lines_k = dot(fx2[...], jnp.concatenate([high, low], axis=1), 1, 1) + dot(fx_low[...], high, 1, 1)
        for dest in range(Y_DEVS):
            sends[chunk][dest] = lines_k[48 * dest:48 * dest + 48]
        recvs[chunk][me_y] = sends[chunk][me_y]

    def copy_y(chunk, shift):
        dest = (me_y + shift) % Y_DEVS
        return pltpu.make_async_remote_copy(
            src_ref=sends[chunk].at[dest], dst_ref=recvs[chunk].at[me_y],
            send_sem=y_send_sem.at[chunk, shift], recv_sem=y_recv_sem.at[chunk, shift],
            device_id={'ydom': dest}, device_id_type=MESH)

    def start_y(chunk):
        for shift in (2, 1, 3):
            copy_y(chunk, shift).start()

    def wait_y(chunk):
        for shift in (2, 1, 3):
            copy_y(chunk, shift).wait()

    lane = lax.broadcasted_iota(jnp.int32, (KX, 128), 1)

    def regroup(blocks):
        out = list(blocks)
        for first, second in ((0, 2), (1, 3)):
            one, two = out[first], out[second]
            out[first] = jnp.where(lane < 64, one, pltpu.roll(two, 64, 1))
            out[second] = jnp.where(lane < 64, pltpu.roll(one, 64, 1), two)
        for first, second in ((0, 1), (2, 3)):
            one, two = out[first], out[second]
            even = (lane // 32) % 2 == 0
            out[first] = jnp.where(even, one, pltpu.roll(two, 32, 1))
            out[second] = jnp.where(even, pltpu.roll(one, 96, 1), two)
        return out

    def transform_y(chunk):
        recv = recvs[chunk]
        lines_re, lines_im = [], []
        for tile in range(WIDTH[chunk] // 128):
            for part_id, lines in ((0, lines_re), (1, lines_im)):
                lines += regroup([recv[source, KX * part_id:KX * part_id + KX, 128 * tile:128 * tile + 128]
                                  for source in range(Y_DEVS)])
        blocks = BLOCKS[chunk]
        values = jnp.concatenate([jnp.concatenate(lines_re[:blocks], axis=0), jnp.concatenate(lines_im[:blocks], axis=0)], axis=1)
        high, low = split(values)
        lines_k = dot(high, fy_high[...], 1, 0) + dot(high, fy_low[...], 1, 0) + dot(low, fy_high[...], 1, 0)
        first = me_z == 0
        zbuf[me_z, Z_SLOT[chunk] * KX:(Z_SLOT[chunk] + blocks) * KX, :] = jnp.where(first, lines_k[:, :128], lines_k[:, 128:])
        halves[chunk][...] = jnp.where(first, lines_k[:, 128:], lines_k[:, :128])

    def copy_z(chunk):
        return pltpu.make_async_remote_copy(
            src_ref=halves[chunk],
            dst_ref=zbuf.at[me_z, pl.ds(Z_SLOT[chunk] * KX, BLOCKS[chunk] * KX)],
            send_sem=z_send_sem.at[chunk], recv_sem=z_recv_sem.at[chunk],
            device_id={'zdom': 1 - me_z}, device_id_type=MESH)

    rhs_a[...] = jnp.zeros_like(rhs_a)
    rhs_b[...] = jnp.zeros_like(rhs_b)
    ghosts[...] = jnp.zeros_like(ghosts)
    zbuf[:, (Z_SLOTS - 1) * KX:, :] = jnp.zeros((Z_DEVS, KX, 128), F32)

    for chunk in range(4):
        spread(chunk)
        transform_x(chunk)
        if chunk == 0:
            pl.semaphore_wait(barrier, 7)
        start_y(chunk)
        if chunk > 0:
            wait_y(chunk - 1)
            transform_y(chunk - 1)
            copy_z(chunk - 1).start()
    wait_y(3)
    transform_y(3)
    copy_z(3).start()
    for chunk in range(4):
        copy_z(chunk).wait()

    sum_rows = jnp.zeros((8, 128), F32)
    for index in range(KX):
        rows = jnp.concatenate([zbuf[source, pl.ds(index, Z_SLOTS, stride=KX), :] for source in range(Z_DEVS)], axis=0)
        high, low = split(rows)
        lines_k = dot(high, fz_high[...], 0, 0) + dot(high, fz_low[...], 0, 0) + dot(low, fz_high[...], 0, 0)
        real = lines_k[0:KY, 0:G] + lines_k[KY:2 * KY, 128:128 + G]
        imag = lines_k[KY:2 * KY, 0:G] - lines_k[0:KY, 128:128 + G]
        energy = 0.5 * influence[index] * (real * real + imag * imag)
        mode_out[index] = energy
        for row in range(0, KY, 8):
            sum_rows = sum_rows + jnp.pad(energy[row:row + 8], ((0, 0), (0, 128 - G)))
    part[...] = jnp.broadcast_to(jnp.sum(sum_rows), (8, 128))
    parts[me] = part[...]

    def copy_e(shift):
        return pltpu.make_async_remote_copy(
            src_ref=part, dst_ref=parts.at[me], send_sem=e_send_sem.at[shift], recv_sem=e_recv_sem.at[shift],
            device_id=device((me + shift) % 8), device_id_type=MESH)

    for shift in range(1, 8):
        copy_e(shift).start()
    for shift in range(1, 8):
        copy_e(shift).wait()
    result = parts[0]
    for rank in range(1, 8):
        result = result + parts[rank]
    energy_out[...] = result * (1.0 / (G * G * G))


def solution(mesh):
    slot_spec = P(('sys', 'ydom', 'zdom'))
    mode_spec = P(('sys', 'ydom'), 'zdom', None)
    tables = dft_x() + dft_y() + dft_z()

    def local_energy(charge, real_mask, grid_idx, spline_w, influence):
        slots = charge.shape[0]
        vmem = pl.BlockSpec(memory_space=pltpu.VMEM)
        mode_energy, energy = pl.pallas_call(
            kernel,
            out_shape=(jax.ShapeDtypeStruct((KX, KY, G), F32), jax.ShapeDtypeStruct((8, 128), F32)),
            in_specs=[vmem] * 11,
            out_specs=(vmem, vmem),
            scratch_shapes=[
                pltpu.VMEM((G, slots), F32),
                pltpu.VMEM((5, 2, 16, slots), BF16),
                pltpu.VMEM((8, slots), F32),
                pltpu.VMEM((2 * ROWS[0], STEP), BF16),
                pltpu.VMEM((2 * ROWS[0], STEP), BF16),
                pltpu.VMEM((256, STEP), BF16),
                pltpu.VMEM((256, STEP), BF16),
                pltpu.VMEM((ROWS[0], 256), F32),
                pltpu.VMEM((384, 128), F32),
                pltpu.VMEM((128, 128), F32),
            ] + [pltpu.VMEM((Y_DEVS, 2 * KX, width), F32) for width in WIDTH] * 2
            + [pltpu.VMEM((blocks * KX, 128), F32) for blocks in BLOCKS] + [
                pltpu.VMEM((Z_DEVS, Z_SLOTS * KX, 128), F32),
                pltpu.VMEM((8, 128), F32),
                pltpu.VMEM((8, 8, 128), F32),
                pltpu.SemaphoreType.DMA((4, 4)),
                pltpu.SemaphoreType.DMA((4, 4)),
                pltpu.SemaphoreType.DMA((4,)),
                pltpu.SemaphoreType.DMA((4,)),
                pltpu.SemaphoreType.DMA((8,)),
                pltpu.SemaphoreType.DMA((8,)),
            ],
            compiler_params=pltpu.CompilerParams(
                collective_id=0, has_side_effects=True, vmem_limit_bytes=60 * 1024 * 1024),
        )(charge.reshape(1, slots), real_mask.reshape(1, slots), grid_idx.T, jnp.transpose(spline_w, (1, 2, 0)),
          influence, *[jnp.asarray(table) for table in tables])
        return mode_energy, energy[0, 0:1]

    return jax.shard_map(local_energy, mesh=mesh, in_specs=(slot_spec, slot_spec, P(('sys', 'ydom', 'zdom'), None), P(('sys', 'ydom', 'zdom'), None, None), mode_spec), out_specs=(mode_spec, P('sys')), check_vma=False)
```

```python
import functools
import math
import jax
import jax.numpy as jnp
import numpy as np
from jax import lax
from jax.experimental import pallas as pl
from jax.experimental.pallas import tpu as pltpu
from jax.sharding import PartitionSpec as P

MESH = pl.DeviceIdType.MESH
F32 = jnp.float32
BF16 = jnp.bfloat16
G = 96
Y_DEVS = 4
Z_DEVS = 2
LEN_Y = 24
LEN_Z = 48
KX = 24
KY = 48
STEP = 1024
UNROLL = 8
PART = 1024
PREP = 512
ROWS = (368, 368, 368, 336)
GHOST_ROW = (320, 320, 320, 288)
BLOCKS = (12, 12, 12, 3, 4, 4, 4)
WIDTH = (384, 384, 384, 128, 128, 128, 128)
GHOSTS = 3
LAST = (4, 5, 6)
SLOT = (0, 12, 24, 12, 0, 4, 8)
EARLY = 36
LATE = 16


def split_np(values):
    high = np.asarray(values, np.float32).astype(jnp.bfloat16)
    low = (np.asarray(values, np.float64) - high.astype(np.float64)).astype(jnp.bfloat16)
    return high, low


def dft_x():
    table = np.zeros((Y_DEVS, 2, KX, 128))
    for dest in range(Y_DEVS):
        angle = 2 * math.pi * (np.outer(np.arange(KX) + KX * dest, np.arange(G)) % G) / G
        table[dest, 0, :, :G] = np.cos(angle)
        table[dest, 1, :, :G] = -np.sin(angle)
    high, low = split_np(table.reshape(Y_DEVS * 2 * KX, 128))
    return np.concatenate([high, high], axis=1), low


def dft_y():
    table = np.zeros((2, Y_DEVS, 32, Z_DEVS, 128))
    for source in range(Y_DEVS):
        y_pos = LEN_Y * source + np.arange(LEN_Y + 3)
        for dest in range(Z_DEVS):
            angle = 2 * math.pi * (np.outer(y_pos, np.arange(KY) + KY * dest) % G) / G
            table[0, source, :LEN_Y + 3, dest, :KY] = np.cos(angle)
            table[1, source, :LEN_Y + 3, dest, :KY] = np.sin(angle)
            table[0, source, :LEN_Y + 3, dest, KY:2 * KY] = -np.sin(angle)
            table[1, source, :LEN_Y + 3, dest, KY:2 * KY] = np.cos(angle)
    return split_np(table.reshape(2 * Y_DEVS * 32, Z_DEVS * 128))


def dft_z(messages, slots):
    table = np.zeros((Z_DEVS, slots, 2, 128))
    for source in range(Z_DEVS):
        for message in messages:
            for block in range(BLOCKS[message]):
                if message == GHOSTS:
                    z_pos = LEN_Z + block
                elif message in LAST:
                    z_pos = 4 * (4 * (message - LAST[0]) + block) + 3
                else:
                    z_pos = 4 * block + message
                angle = 2 * math.pi * (((z_pos + LEN_Z * source) * np.arange(G)) % G) / G
                table[source, SLOT[message] + block, 0, :G] = np.cos(angle)
                table[source, SLOT[message] + block, 1, :G] = np.sin(angle)
    return split_np(table.reshape(Z_DEVS * slots, 256))


def split(values):
    high = values.astype(BF16)
    return high, (values - high.astype(F32)).astype(BF16)


def dot(lhs, rhs, lhs_dim, rhs_dim):
    return lax.dot_general(lhs, rhs, (((lhs_dim,), (rhs_dim,)), ((), ())), preferred_element_type=F32)


def kernel(charge, mask, grid_idx, spline_w, influence_in, fx2_in, fx_low_in, fy_high_in, fy_low_in, early_high_in,
           early_low_in, late_in, mode_out, energy_out,
           influence, fx2, fx_low, fy_high, fy_low, early_high, early_low, late, mode,
           line_y, taps, base, lhs_a, lhs_b, rhs_a, rhs_b, total, packed, ghosts, *more):
    slots = charge.shape[1]
    me_y = lax.axis_index('ydom')
    me_z = lax.axis_index('zdom')
    me = me_z * Y_DEVS + me_y
    count = len(BLOCKS)
    sends, recvs, halves = more[:count], more[count:2 * count], more[2 * count:3 * count]
    (z_early, z_late, sums, part, parts,
     y_send_sem, y_recv_sem, z_send_sem, z_recv_sem, e_send_sem, e_recv_sem, in_sem, out_sem) = more[3 * count:]

    loads = [pltpu.make_async_copy(source, dest, in_sem.at[index]) for index, (source, dest) in enumerate((
        (fx2_in, fx2), (fx_low_in, fx_low), (fy_high_in, fy_high), (fy_low_in, fy_low), (early_high_in, early_high),
        (early_low_in, early_low), (late_in, late), (influence_in, influence)))]
    for load in loads:
        load.start()

    def device(rank):
        return {'zdom': rank // Y_DEVS, 'ydom': rank % Y_DEVS}

    barrier = pltpu.get_barrier_semaphore()
    for shift in range(1, 8):
        pl.semaphore_signal(barrier, inc=1, device_id=device((me + shift) % 8), device_id_type=MESH)

    row4 = lax.broadcasted_iota(jnp.int32, (4, PREP), 0)
    row16 = lax.broadcasted_iota(jnp.int32, (16, PART), 0)
    row40 = lax.broadcasted_iota(jnp.int32, (40, PREP), 0)
    row40 = jnp.where(row40 < 32, row40, row40 % 4 + 24)
    row16_f = row16.astype(F32)

    def prepare(start):
        at = pl.ds(start, PREP)
        base_x, base_y, base_z = grid_idx[0:1, at], grid_idx[1:2, at], grid_idx[2:3, at]
        weight = charge[0:1, at] * mask[0:1, at].astype(F32)
        values = jnp.zeros((40, PREP), F32)
        for tap in range(4):
            values = jnp.where(row40 == base_y + tap, spline_w[1, tap:tap + 1, at], values)
        high = values.astype(BF16).astype(F32)
        for half, lines in ((0, high), (1, values - high)):
            for index, (top, bottom) in enumerate(((0, 1), (2, 0), (1, 2), (4, 4), (2, 3))):
                line_y[index, half, :, at] = jnp.concatenate(
                    [lines[8 * top:8 * top + 8], lines[8 * bottom:8 * bottom + 8]], axis=0).astype(BF16)
        tap = (row4 - base_z) & 3
        values = jnp.where(tap < 2, jnp.where(tap == 0, spline_w[2, 0:1, at], spline_w[2, 1:2, at]),
                           jnp.where(tap == 2, spline_w[2, 2:3, at], spline_w[2, 3:4, at]))
        base[0:4, at] = ((base_z + tap) >> 2).astype(F32)
        base[4:5, at] = base_x.astype(F32)
        weight_x = spline_w[0, :, at] * weight
        for chunk in range(4):
            product = weight_x * values[chunk:chunk + 1]
            high = product.astype(BF16).astype(F32)
            taps[chunk, 0:4, at] = high
            taps[chunk, 4:8, at] = product - high

    def build(chunk, start, to, lhs, rhs):
        at = pl.ds(start, PART)

        def spread_row(values):
            return jnp.broadcast_to(values, (16, PART)).astype(BF16)

        base_x = jnp.broadcast_to(base[4:5, at], (16, PART))
        rows = [spread_row(taps[chunk, index:index + 1, at]) for index in range(8)]
        zero = jnp.zeros((16, PART), BF16)
        offset = (row16_f - base_x).astype(BF16)
        wrapped = jnp.where(offset < jnp.asarray(-90, BF16), offset + jnp.asarray(G, BF16), offset)
        for group in range(G // 16):
            high, low = zero, zero
            for tap in range(4):
                hit = (offset if group else wrapped) == jnp.asarray(tap - 16 * group, BF16)
                high = jnp.where(hit, rows[tap], high)
                low = jnp.where(hit, rows[4 + tap], low)
            rhs[16 * group:16 * group + 16, to:to + PART] = high
            rhs[128 + 16 * group:144 + 16 * group, to:to + PART] = low
        block = jnp.broadcast_to(base[chunk:chunk + 1, at], (16, PART))
        block_a = block.astype(BF16)
        block_b = (block - (row16 // 8).astype(F32)).astype(BF16)
        block_g = (block - (row16 // 4).astype(F32)).astype(BF16)
        tiles = []
        for pair in range(6):
            tiles += [(block_a, 2 * pair, 0), (block_b, 2 * pair, 1), (block_a, 2 * pair + 1, 2)]
        if chunk < 3:
            tiles += [(block_a, 12, 0), (block_a, 12, 4)]
        tiles += [(block_g, 0, 3), (block_g, 4, 3), (block_g, 8, 3)]
        for index, (source, value, pattern) in enumerate(tiles):
            hit = source == jnp.asarray(value, BF16)
            for half in range(2):
                lhs[half * ROWS[chunk] + 16 * index:half * ROWS[chunk] + 16 * index + 16, to:to + PART] = jnp.where(
                    hit, line_y[pattern, half, :, at], zero)

    def spread(chunk, first, last):
        rows = ROWS[chunk]

        def fill(step, lhs, rhs):
            start = pl.multiple_of(jnp.minimum(step, slots // STEP - 1) * STEP, STEP)
            for to in range(0, STEP, PART):
                build(chunk, start + to, to, lhs, rhs)

        def add(lhs, rhs):
            product = dot(lhs[0:2 * rows, :], rhs[...], 1, 1)
            total[0:rows, :] += product[:rows] + product[rows:]

        if first == 0:
            total[...] = jnp.zeros_like(total)
            fill(0, lhs_a, rhs_a)

        def body(pair, carry):
            add(lhs_a, rhs_a)
            fill(2 * pair + 1, lhs_b, rhs_b)
            add(lhs_b, rhs_b)
            fill(2 * pair + 2, lhs_a, rhs_a)
            return carry

        lax.fori_loop(first, last, body, 0)

    row8 = lax.broadcasted_iota(jnp.int32, (8, 128), 0)

    def pack(chunk, first, last):
        def lines(start, rows):
            return total[start:start + rows, 0:128] + total[start:start + rows, 128:256]

        for pair in range(first, last):
            ghost = lines(GHOST_ROW[chunk] + 8 * pair, 8)
            packed[64 * pair:64 * pair + 24, :] = lines(48 * pair, 24)
            packed[64 * pair + 24:64 * pair + 32, :] = jnp.where(row8 < 4, ghost, 0.0)
            packed[64 * pair + 32:64 * pair + 56, :] = lines(48 * pair + 24, 24)
            packed[64 * pair + 56:64 * pair + 64, :] = jnp.where(row8 < 4, pltpu.roll(ghost, 4, 0), 0.0)
        if chunk < 3:
            ghosts[32 * chunk:32 * chunk + 32, :] = lines(288, 32)

    def transform_x(message, values):
        high, low = split(values)
        lines_k = dot(fx2[...], jnp.concatenate([high, low], axis=1), 1, 1) + dot(fx_low[...], high, 1, 1)
        for dest in range(Y_DEVS):
            sends[message][dest] = lines_k[48 * dest:48 * dest + 48]
        recvs[message][me_y] = sends[message][me_y]

    def copy_y(chunk, shift):
        dest = (me_y + shift) % Y_DEVS
        return pltpu.make_async_remote_copy(
            src_ref=sends[chunk].at[dest], dst_ref=recvs[chunk].at[me_y],
            send_sem=y_send_sem.at[chunk, shift], recv_sem=y_recv_sem.at[chunk, shift],
            device_id={'ydom': dest}, device_id_type=MESH)

    def start_y(chunk):
        for shift in (2, 1, 3):
            copy_y(chunk, shift).start()

    def wait_y(chunk):
        for shift in (2, 1, 3):
            copy_y(chunk, shift).wait()

    lane = lax.broadcasted_iota(jnp.int32, (KX, 128), 1)

    def regroup(blocks):
        out = list(blocks)
        for first, second in ((0, 2), (1, 3)):
            one, two = out[first], out[second]
            out[first] = jnp.where(lane < 64, one, pltpu.roll(two, 64, 1))
            out[second] = jnp.where(lane < 64, pltpu.roll(one, 64, 1), two)
        for first, second in ((0, 1), (2, 3)):
            one, two = out[first], out[second]
            even = (lane // 32) % 2 == 0
            out[first] = jnp.where(even, one, pltpu.roll(two, 32, 1))
            out[second] = jnp.where(even, pltpu.roll(one, 96, 1), two)
        return out

    def z_rows(message):
        per_source = EARLY if message < GHOSTS else LATE
        return pl.ds((me_z * per_source + SLOT[message]) * KX, BLOCKS[message] * KX)

    def z_buffer(message):
        return z_early if message < GHOSTS else z_late

    def copy_z(message):
        return pltpu.make_async_remote_copy(
            src_ref=halves[message], dst_ref=z_buffer(message).at[z_rows(message)],
            send_sem=z_send_sem.at[message], recv_sem=z_recv_sem.at[message],
            device_id={'zdom': 1 - me_z}, device_id_type=MESH)

    def transform_y(message):
        wait_y(message)
        recv = recvs[message]
        lines_re, lines_im = [], []
        for tile in range(WIDTH[message] // 128):
            for part_id, lines in ((0, lines_re), (1, lines_im)):
                lines += regroup([recv[source, KX * part_id:KX * part_id + KX, 128 * tile:128 * tile + 128]
                                  for source in range(Y_DEVS)])
        blocks = BLOCKS[message]
        values = jnp.concatenate([jnp.concatenate(lines_re[:blocks], axis=0), jnp.concatenate(lines_im[:blocks], axis=0)], axis=1)
        high, low = split(values)
        lines_k = dot(high, fy_high[...], 1, 0) + dot(high, fy_low[...], 1, 0) + dot(low, fy_high[...], 1, 0)
        first = me_z == 0
        halves[message][...] = jnp.where(first, lines_k[:, 128:], lines_k[:, :128])
        z_buffer(message)[z_rows(message), :] = jnp.where(first, lines_k[:, :128], lines_k[:, 128:])
        copy_z(message).start()

    rhs_a[...] = jnp.zeros_like(rhs_a)
    rhs_b[...] = jnp.zeros_like(rhs_b)
    ghosts[...] = jnp.zeros_like(ghosts)
    for source in range(Z_DEVS):
        z_late[((source + 1) * LATE - 1) * KX:(source + 1) * LATE * KX, :] = jnp.zeros((KX, 128), F32)

    def prepare_step(step, carry):
        prepare(pl.multiple_of(step * PREP, PREP))
        return carry

    lax.fori_loop(0, slots // PREP, prepare_step, 0)

    steps = slots // STEP // 2
    for chunk in range(3):
        spread(chunk, 0, steps)
        pack(chunk, 0, 6)
        if chunk == 0:
            for load in loads:
                load.wait()
        transform_x(chunk, packed[...])
        if chunk == 0:
            pl.semaphore_wait(barrier, 7)
        start_y(chunk)
        if chunk == 2:
            transform_x(GHOSTS, ghosts[...])
            start_y(GHOSTS)
        if chunk > 0:
            transform_y(chunk - 1)
    spread(3, 0, steps - 2)
    transform_y(2)
    spread(3, steps - 2, steps)
    for index, message in enumerate(LAST):
        pack(3, 2 * index, 2 * index + 2)
        transform_x(message, packed[128 * index:128 * index + 128, :])
        start_y(message)
    transform_y(GHOSTS)
    for message in range(3):
        copy_z(message).wait()
    def sum_early(index, carry):
        high, low = split(z_early[pl.ds(index, Z_DEVS * EARLY, stride=KX), :])
        high, low = high[:, :2 * KY], low[:, :2 * KY]
        sums[index] = dot(high, early_high[...], 0, 0) + dot(high, early_low[...], 0, 0) + dot(low, early_high[...], 0, 0)
        return carry

    lax.fori_loop(0, KX, sum_early, 0, unroll=UNROLL)
    for message in LAST:
        transform_y(message)
    for message in (GHOSTS,) + LAST:
        copy_z(message).wait()

    def copy_out(index):
        rows = pl.ds(8 * index, 8)
        return pltpu.make_async_copy(mode.at[rows], mode_out.at[rows], out_sem.at[index])

    def sum_late(index, energy_sum):
        high, low = split(z_late[pl.ds(index, Z_DEVS * LATE, stride=KX), :])
        values = jnp.concatenate([high, low, high], axis=0)[:, :2 * KY]
        lines_k = sums[index] + dot(values, late[...], 0, 0)
        real = lines_k[0:KY, 0:G] + lines_k[KY:2 * KY, 128:128 + G]
        imag = lines_k[KY:2 * KY, 0:G] - lines_k[0:KY, 128:128 + G]
        energy = 0.5 * influence[index] * (real * real + imag * imag)
        mode[index] = energy
        return energy_sum + energy

    energy_sum = jnp.zeros((KY, G), F32)
    for index in range(3):
        energy_sum = lax.fori_loop(8 * index, 8 * index + 8, sum_late, energy_sum, unroll=UNROLL)
        copy_out(index).start()
    part[...] = jnp.broadcast_to(jnp.sum(energy_sum), (8, 128))
    parts[me] = part[...]

    def copy_e(shift):
        return pltpu.make_async_remote_copy(
            src_ref=part, dst_ref=parts.at[me], send_sem=e_send_sem.at[shift], recv_sem=e_recv_sem.at[shift],
            device_id=device((me + shift) % 8), device_id_type=MESH)

    for shift in range(1, 8):
        copy_e(shift).start()
    for shift in range(1, 8):
        copy_e(shift).wait()
    result = parts[0]
    for rank in range(1, 8):
        result = result + parts[rank]
    energy_out[...] = result * (1.0 / (G * G * G))
    for index in range(3):
        copy_out(index).wait()


def solution(mesh):
    slot_spec = P(('sys', 'ydom', 'zdom'))
    mode_spec = P(('sys', 'ydom'), 'zdom', None)
    late_high, late_low = dft_z((GHOSTS,) + LAST, LATE)
    tables = dft_x() + dft_y() + dft_z((0, 1, 2), EARLY) + (np.concatenate([late_high, late_high, late_low], axis=0),)

    def local_energy(charge, real_mask, grid_idx, spline_w, influence):
        slots = charge.shape[0]
        vmem = pl.BlockSpec(memory_space=pltpu.VMEM)
        whole = pl.BlockSpec(memory_space=pl.ANY)
        mode_energy, energy = pl.pallas_call(
            kernel,
            out_shape=(jax.ShapeDtypeStruct((KX, KY, G), F32), jax.ShapeDtypeStruct((8, 128), F32)),
            in_specs=[vmem] * 4 + [whole] * (1 + len(tables)),
            out_specs=(whole, vmem),
            scratch_shapes=[
                pltpu.VMEM(influence.shape, F32),
            ] + [pltpu.VMEM(table.shape, BF16) for table in tables] + [
                pltpu.VMEM((KX, KY, G), F32),
                pltpu.VMEM((5, 2, 16, slots), BF16),
                pltpu.VMEM((4, 8, slots), F32),
                pltpu.VMEM((8, slots), F32),
                pltpu.VMEM((2 * ROWS[0], STEP), BF16),
                pltpu.VMEM((2 * ROWS[0], STEP), BF16),
                pltpu.VMEM((256, STEP), BF16),
                pltpu.VMEM((256, STEP), BF16),
                pltpu.VMEM((ROWS[0], 256), F32),
                pltpu.VMEM((384, 128), F32),
                pltpu.VMEM((128, 128), F32),
            ] + [pltpu.VMEM((Y_DEVS, 2 * KX, width), F32) for width in WIDTH] * 2
            + [pltpu.VMEM((blocks * KX, 128), F32) for blocks in BLOCKS] + [
                pltpu.VMEM((Z_DEVS * EARLY * KX, 128), F32),
                pltpu.VMEM((Z_DEVS * LATE * KX, 128), F32),
                pltpu.VMEM((KX, 2 * KY, 256), F32),
                pltpu.VMEM((8, 128), F32),
                pltpu.VMEM((8, 8, 128), F32),
                pltpu.SemaphoreType.DMA((len(BLOCKS), 4)),
                pltpu.SemaphoreType.DMA((len(BLOCKS), 4)),
                pltpu.SemaphoreType.DMA((len(BLOCKS),)),
                pltpu.SemaphoreType.DMA((len(BLOCKS),)),
                pltpu.SemaphoreType.DMA((8,)),
                pltpu.SemaphoreType.DMA((8,)),
                pltpu.SemaphoreType.DMA((8,)),
                pltpu.SemaphoreType.DMA((3,)),
            ],
            compiler_params=pltpu.CompilerParams(
                collective_id=0, has_side_effects=True, vmem_limit_bytes=60 * 1024 * 1024),
        )(charge.reshape(1, slots), real_mask.reshape(1, slots), grid_idx.T, jnp.transpose(spline_w, (1, 2, 0)),
          influence, *[jnp.asarray(table) for table in tables])
        return mode_energy, energy[0, 0:1]

    return jax.shard_map(local_energy, mesh=mesh, in_specs=(slot_spec, slot_spec, P(('sys', 'ydom', 'zdom'), None), P(('sys', 'ydom', 'zdom'), None, None), mode_spec), out_specs=(mode_spec, P('sys')), check_vma=False)
```

```python
import functools
import math
import jax
import jax.numpy as jnp
import numpy as np
from jax import lax
from jax.experimental import pallas as pl
from jax.experimental.pallas import tpu as pltpu
from jax.sharding import PartitionSpec as P

MESH = pl.DeviceIdType.MESH
F32 = jnp.float32
BF16 = jnp.bfloat16
G = 96
Y_DEVS = 4
Z_DEVS = 2
LEN_Y = 24
LEN_Z = 48
KX = 24
KY = 48
STEP = 2048
SECTIONS = 4
UNROLL = 8
PART = 1024
PREP = 512
ROWS = (368, 368, 368, 336)
GHOST_ROW = (320, 320, 320, 288)
BLOCKS = (4,) * 12 + (3,)
GHOSTS = 12
SLOT = (0, 4, 8, 12, 16, 20, 24, 28, 32, 0, 4, 8, 12)
EARLY = 36
LATE = 16


def split_np(values):
    high = np.asarray(values, np.float32).astype(jnp.bfloat16)
    low = (np.asarray(values, np.float64) - high.astype(np.float64)).astype(jnp.bfloat16)
    return high, low


def dft_x():
    table = np.zeros((Y_DEVS, 2, KX, 128))
    for dest in range(Y_DEVS):
        angle = 2 * math.pi * (np.outer(np.arange(KX) + KX * dest, np.arange(G)) % G) / G
        table[dest, 0, :, :G] = np.cos(angle)
        table[dest, 1, :, :G] = -np.sin(angle)
    high, low = split_np(table.reshape(Y_DEVS * 2 * KX, 128))
    return np.concatenate([high, high], axis=1), low


def dft_y():
    table = np.zeros((2, Y_DEVS, 32, Z_DEVS, 128))
    for source in range(Y_DEVS):
        y_pos = LEN_Y * source + np.arange(LEN_Y + 3)
        for dest in range(Z_DEVS):
            angle = 2 * math.pi * (np.outer(y_pos, np.arange(KY) + KY * dest) % G) / G
            table[0, source, :LEN_Y + 3, dest, :KY] = np.cos(angle)
            table[1, source, :LEN_Y + 3, dest, :KY] = np.sin(angle)
            table[0, source, :LEN_Y + 3, dest, KY:2 * KY] = -np.sin(angle)
            table[1, source, :LEN_Y + 3, dest, KY:2 * KY] = np.cos(angle)
    return split_np(table.reshape(2 * Y_DEVS * 32, Z_DEVS * 128))


def dft_z(messages, slots):
    table = np.zeros((Z_DEVS, slots, 2, 128))
    for source in range(Z_DEVS):
        for message in messages:
            for block in range(BLOCKS[message]):
                if message == GHOSTS:
                    z_pos = LEN_Z + block
                else:
                    z_pos = 4 * (4 * (message % 3) + block) + message // 3
                angle = 2 * math.pi * (((z_pos + LEN_Z * source) * np.arange(G)) % G) / G
                table[source, SLOT[message] + block, 0, :G] = np.cos(angle)
                table[source, SLOT[message] + block, 1, :G] = np.sin(angle)
    return split_np(table.reshape(Z_DEVS * slots, 256))


def split(values):
    high = values.astype(BF16)
    return high, (values - high.astype(F32)).astype(BF16)


def dot(lhs, rhs, lhs_dim, rhs_dim):
    return lax.dot_general(lhs, rhs, (((lhs_dim,), (rhs_dim,)), ((), ())), preferred_element_type=F32)


def kernel(charge_in, mask_in, grid_idx_in, spline_w_in, influence_in, fx2_in, fx_low_in, fy_high_in, fy_low_in, early_high_in,
           early_low_in, late_in, mode, energy_out,
           charge, mask, grid_idx, spline_w, influence, fx2, fx_low, fy_high, fy_low, early_high, early_low, late,
           line_y, taps, base, lhs_a, lhs_b, rhs_a, rhs_b, total, packed, ghosts, *more):
    slots = charge.shape[1]
    me_y = lax.axis_index('ydom')
    me_z = lax.axis_index('zdom')
    me = me_z * Y_DEVS + me_y
    count = len(BLOCKS)
    sends, recvs, halves = more[:count], more[count:2 * count], more[2 * count:3 * count]
    (z_early, z_late, sums, part, parts,
     y_send_sem, y_recv_sem, z_send_sem, z_recv_sem, e_send_sem, e_recv_sem, in_sem, slot_sem) = more[3 * count:]

    def section(index):
        at = pl.ds(index * (slots // SECTIONS), slots // SECTIONS)
        return [pltpu.make_async_copy(source.at[..., at], dest.at[..., at], slot_sem.at[index, number])
                for number, (source, dest) in enumerate((
                    (charge_in, charge), (mask_in, mask), (grid_idx_in, grid_idx), (spline_w_in, spline_w)))]

    for index in range(SECTIONS):
        for load in section(index):
            load.start()
    loads = [pltpu.make_async_copy(source, dest, in_sem.at[index]) for index, (source, dest) in enumerate((
        (fx2_in, fx2), (fx_low_in, fx_low), (fy_high_in, fy_high), (fy_low_in, fy_low), (early_high_in, early_high),
        (early_low_in, early_low), (late_in, late), (influence_in, influence)))]
    for load in loads:
        load.start()

    def device(rank):
        return {'zdom': rank // Y_DEVS, 'ydom': rank % Y_DEVS}

    barrier = pltpu.get_barrier_semaphore()
    for shift in range(1, 8):
        pl.semaphore_signal(barrier, inc=1, device_id=device((me + shift) % 8), device_id_type=MESH)

    row4 = lax.broadcasted_iota(jnp.int32, (4, PREP), 0)
    row16 = lax.broadcasted_iota(jnp.int32, (16, PART), 0)
    row40 = lax.broadcasted_iota(jnp.int32, (40, PREP), 0)
    row40 = jnp.where(row40 < 32, row40, row40 % 4 + 24)
    row16_f = row16.astype(F32)

    def prepare(start):
        at = pl.ds(start, PREP)
        base_x, base_y, base_z = grid_idx[0:1, at], grid_idx[1:2, at], grid_idx[2:3, at]
        weight = charge[0:1, at] * mask[0:1, at].astype(F32)
        values = jnp.zeros((40, PREP), F32)
        for tap in range(4):
            values = jnp.where(row40 == base_y + tap, spline_w[1, tap:tap + 1, at], values)
        high = values.astype(BF16).astype(F32)
        for half, lines in ((0, high), (1, values - high)):
            for index, (top, bottom) in enumerate(((0, 1), (2, 0), (1, 2), (4, 4), (2, 3))):
                line_y[index, half, :, at] = jnp.concatenate(
                    [lines[8 * top:8 * top + 8], lines[8 * bottom:8 * bottom + 8]], axis=0).astype(BF16)
        tap = (row4 - base_z) & 3
        values = jnp.where(tap < 2, jnp.where(tap == 0, spline_w[2, 0:1, at], spline_w[2, 1:2, at]),
                           jnp.where(tap == 2, spline_w[2, 2:3, at], spline_w[2, 3:4, at]))
        base[0:4, at] = ((base_z + tap) >> 2).astype(F32)
        base[4:5, at] = base_x.astype(F32)
        weight_x = spline_w[0, :, at] * weight
        for chunk in range(4):
            product = weight_x * values[chunk:chunk + 1]
            high = product.astype(BF16).astype(F32)
            taps[chunk, 0:4, at] = high
            taps[chunk, 4:8, at] = product - high

    def build(chunk, start, to, lhs, rhs):
        at = pl.ds(start, PART)

        def spread_row(values):
            return jnp.broadcast_to(values, (16, PART)).astype(BF16)

        base_x = jnp.broadcast_to(base[4:5, at], (16, PART))
        rows = [spread_row(taps[chunk, index:index + 1, at]) for index in range(8)]
        zero = jnp.zeros((16, PART), BF16)
        offset = (row16_f - base_x).astype(BF16)
        wrapped = jnp.where(offset < jnp.asarray(-90, BF16), offset + jnp.asarray(G, BF16), offset)
        for group in range(G // 16):
            high, low = zero, zero
            for tap in range(4):
                hit = (offset if group else wrapped) == jnp.asarray(tap - 16 * group, BF16)
                high = jnp.where(hit, rows[tap], high)
                low = jnp.where(hit, rows[4 + tap], low)
            rhs[16 * group:16 * group + 16, to:to + PART] = high
            rhs[128 + 16 * group:144 + 16 * group, to:to + PART] = low
        block = jnp.broadcast_to(base[chunk:chunk + 1, at], (16, PART))
        block_a = block.astype(BF16)
        block_b = (block - (row16 // 8).astype(F32)).astype(BF16)
        block_g = (block - (row16 // 4).astype(F32)).astype(BF16)
        tiles = []
        for pair in range(6):
            tiles += [(block_a, 2 * pair, 0), (block_b, 2 * pair, 1), (block_a, 2 * pair + 1, 2)]
        if chunk < 3:
            tiles += [(block_a, 12, 0), (block_a, 12, 4)]
        tiles += [(block_g, 0, 3), (block_g, 4, 3), (block_g, 8, 3)]
        for index, (source, value, pattern) in enumerate(tiles):
            hit = source == jnp.asarray(value, BF16)
            for half in range(2):
                lhs[half * ROWS[chunk] + 16 * index:half * ROWS[chunk] + 16 * index + 16, to:to + PART] = jnp.where(
                    hit, line_y[pattern, half, :, at], zero)

    def spread(chunk, first, last):
        rows = ROWS[chunk]

        def fill(step, lhs, rhs):
            start = pl.multiple_of(jnp.minimum(step, slots // STEP - 1) * STEP, STEP)
            for to in range(0, STEP, PART):
                build(chunk, start + to, to, lhs, rhs)

        def add(lhs, rhs):
            product = dot(lhs[0:2 * rows, :], rhs[...], 1, 1)
            total[0:rows, :] += product[:rows] + product[rows:]

        if first == 0:
            total[...] = jnp.zeros_like(total)
            fill(0, lhs_a, rhs_a)

        def body(pair, carry):
            add(lhs_a, rhs_a)
            fill(2 * pair + 1, lhs_b, rhs_b)
            add(lhs_b, rhs_b)
            fill(2 * pair + 2, lhs_a, rhs_a)
            return carry

        lax.fori_loop(first, last, body, 0)

    row8 = lax.broadcasted_iota(jnp.int32, (8, 128), 0)

    def pack(chunk, first, last):
        def lines(start, rows):
            return total[start:start + rows, 0:128] + total[start:start + rows, 128:256]

        for pair in range(first, last):
            ghost = lines(GHOST_ROW[chunk] + 8 * pair, 8)
            packed[64 * pair:64 * pair + 24, :] = lines(48 * pair, 24)
            packed[64 * pair + 24:64 * pair + 32, :] = jnp.where(row8 < 4, ghost, 0.0)
            packed[64 * pair + 32:64 * pair + 56, :] = lines(48 * pair + 24, 24)
            packed[64 * pair + 56:64 * pair + 64, :] = jnp.where(row8 < 4, pltpu.roll(ghost, 4, 0), 0.0)
        if chunk < 3:
            ghosts[32 * chunk:32 * chunk + 32, :] = lines(288, 32)

    def transform_x(messages, values):
        high, low = split(values)
        lines_k = dot(fx2[...], jnp.concatenate([high, low], axis=1), 1, 1) + dot(fx_low[...], high, 1, 1)
        for index, message in enumerate(messages):
            for dest in range(Y_DEVS):
                sends[message][dest] = lines_k[48 * dest:48 * dest + 48, 128 * index:128 * index + 128]
            recvs[message][me_y] = sends[message][me_y]
        for message in messages:
            start_y(message)

    def copy_y(chunk, shift):
        dest = (me_y + shift) % Y_DEVS
        return pltpu.make_async_remote_copy(
            src_ref=sends[chunk].at[dest], dst_ref=recvs[chunk].at[me_y],
            send_sem=y_send_sem.at[chunk, shift], recv_sem=y_recv_sem.at[chunk, shift],
            device_id={'ydom': dest}, device_id_type=MESH)

    def start_y(chunk):
        for shift in (2, 1, 3):
            copy_y(chunk, shift).start()

    def wait_y(chunk):
        for shift in (2, 1, 3):
            copy_y(chunk, shift).wait()

    lane = lax.broadcasted_iota(jnp.int32, (KX, 128), 1)

    def regroup(blocks):
        out = list(blocks)
        for first, second in ((0, 2), (1, 3)):
            one, two = out[first], out[second]
            out[first] = jnp.where(lane < 64, one, pltpu.roll(two, 64, 1))
            out[second] = jnp.where(lane < 64, pltpu.roll(one, 64, 1), two)
        for first, second in ((0, 1), (2, 3)):
            one, two = out[first], out[second]
            even = (lane // 32) % 2 == 0
            out[first] = jnp.where(even, one, pltpu.roll(two, 32, 1))
            out[second] = jnp.where(even, pltpu.roll(one, 96, 1), two)
        return out

    def is_early(message):
        return message < 9

    def z_rows(message):
        per_source = EARLY if is_early(message) else LATE
        return pl.ds((me_z * per_source + SLOT[message]) * KX, BLOCKS[message] * KX)

    def z_buffer(message):
        return z_early if is_early(message) else z_late

    def copy_z(message):
        return pltpu.make_async_remote_copy(
            src_ref=halves[message], dst_ref=z_buffer(message).at[z_rows(message)],
            send_sem=z_send_sem.at[message], recv_sem=z_recv_sem.at[message],
            device_id={'zdom': 1 - me_z}, device_id_type=MESH)

    def transform_y(*messages):
        lines_re, lines_im = [], []
        for message in messages:
            wait_y(message)
            for part_id, lines in ((0, lines_re), (1, lines_im)):
                lines += regroup([recvs[message][source, KX * part_id:KX * part_id + KX, :]
                                  for source in range(Y_DEVS)])[:BLOCKS[message]]
        values = jnp.concatenate([jnp.concatenate(lines_re, axis=0), jnp.concatenate(lines_im, axis=0)], axis=1)
        high, low = split(values)
        lines_k = dot(high, fy_high[...], 1, 0) + dot(high, fy_low[...], 1, 0) + dot(low, fy_high[...], 1, 0)
        first = me_z == 0
        there = jnp.where(first, lines_k[:, 128:], lines_k[:, :128])
        here = jnp.where(first, lines_k[:, :128], lines_k[:, 128:])
        row = 0
        for message in messages:
            rows = BLOCKS[message] * KX
            halves[message][...] = there[row:row + rows]
            z_buffer(message)[z_rows(message), :] = here[row:row + rows]
            row += rows
        for message in messages:
            copy_z(message).start()

    rhs_a[...] = jnp.zeros_like(rhs_a)
    rhs_b[...] = jnp.zeros_like(rhs_b)
    ghosts[...] = jnp.zeros_like(ghosts)
    for source in range(Z_DEVS):
        z_late[((source + 1) * LATE - 1) * KX:(source + 1) * LATE * KX, :] = jnp.zeros((KX, 128), F32)

    def prepare_step(step, carry):
        prepare(pl.multiple_of(step * PREP, PREP))
        return carry

    part_steps = slots // PREP // SECTIONS
    for index in range(SECTIONS):
        for load in section(index):
            load.wait()
        lax.fori_loop(index * part_steps, (index + 1) * part_steps, prepare_step, 0)

    steps = slots // STEP // 2
    for chunk in range(3):
        spread(chunk, 0, steps)
        pack(chunk, 0, 6)
        if chunk == 0:
            for load in loads:
                load.wait()
            pl.semaphore_wait(barrier, 7)
        transform_x(range(3 * chunk, 3 * chunk + 3), packed[...])
        if chunk == 2:
            transform_x((GHOSTS,), ghosts[...])
        if chunk > 0:
            transform_y(*range(3 * chunk - 3, 3 * chunk))
    spread(3, 0, steps - 2)
    transform_y(6)
    spread(3, steps - 2, steps - 1)
    transform_y(7)
    spread(3, steps - 1, steps)
    for index in range(3):
        pack(3, 2 * index, 2 * index + 2)
        transform_x((9 + index,), packed[128 * index:128 * index + 128, :])
    transform_y(8, GHOSTS)
    for message in range(9):
        copy_z(message).wait()
    def sum_early(index, carry):
        high, low = split(z_early[pl.ds(index, Z_DEVS * EARLY, stride=KX), :])
        high, low = high[:, :2 * KY], low[:, :2 * KY]
        sums[index] = dot(high, early_high[...], 0, 0) + dot(high, early_low[...], 0, 0) + dot(low, early_high[...], 0, 0)
        return carry

    lax.fori_loop(0, KX, sum_early, 0, unroll=UNROLL)
    for message in range(9, 12):
        transform_y(message)
    for message in range(9, 13):
        copy_z(message).wait()

    def sum_late(index, energy_sum):
        high, low = split(z_late[pl.ds(index, Z_DEVS * LATE, stride=KX), :])
        values = jnp.concatenate([high, low, high], axis=0)[:, :2 * KY]
        lines_k = sums[index] + dot(values, late[...], 0, 0)
        real = lines_k[0:KY, 0:G] + lines_k[KY:2 * KY, 128:128 + G]
        imag = lines_k[KY:2 * KY, 0:G] - lines_k[0:KY, 128:128 + G]
        energy = 0.5 * influence[index] * (real * real + imag * imag)
        mode[index] = energy
        return energy_sum + energy

    energy_sum = jnp.zeros((KY, G), F32)
    for index in range(3):
        energy_sum = lax.fori_loop(8 * index, 8 * index + 8, sum_late, energy_sum, unroll=UNROLL)
    part[...] = jnp.broadcast_to(jnp.sum(energy_sum), (8, 128))
    parts[me] = part[...]

    def copy_e(shift):
        return pltpu.make_async_remote_copy(
            src_ref=part, dst_ref=parts.at[me], send_sem=e_send_sem.at[shift], recv_sem=e_recv_sem.at[shift],
            device_id=device((me + shift) % 8), device_id_type=MESH)

    for shift in range(1, 8):
        copy_e(shift).start()
    for shift in range(1, 8):
        copy_e(shift).wait()
    result = parts[0]
    for rank in range(1, 8):
        result = result + parts[rank]
    energy_out[...] = result * (1.0 / (G * G * G))


def solution(mesh):
    slot_spec = P(('sys', 'ydom', 'zdom'))
    mode_spec = P(('sys', 'ydom'), 'zdom', None)
    late_high, late_low = dft_z(range(9, 13), LATE)
    tables = dft_x() + dft_y() + dft_z(range(9), EARLY) + (np.concatenate([late_high, late_high, late_low], axis=0),)

    def local_energy(charge, real_mask, grid_idx, spline_w, influence):
        slots = charge.shape[0]
        vmem = pl.BlockSpec(memory_space=pltpu.VMEM)
        whole = pl.BlockSpec(memory_space=pl.ANY)
        mode_energy, energy = pl.pallas_call(
            kernel,
            out_shape=(pltpu.VMEM((KX, KY, G), F32), pltpu.VMEM((8, 128), F32)),
            in_specs=[whole] * (5 + len(tables)),
            out_specs=(vmem, vmem),
            scratch_shapes=[
                pltpu.VMEM((1, slots), F32),
                pltpu.VMEM((1, slots), jnp.int32),
                pltpu.VMEM((3, slots), jnp.int32),
                pltpu.VMEM((3, 4, slots), F32),
                pltpu.VMEM(influence.shape, F32),
            ] + [pltpu.VMEM(table.shape, BF16) for table in tables] + [
                pltpu.VMEM((5, 2, 16, slots), BF16),
                pltpu.VMEM((4, 8, slots), F32),
                pltpu.VMEM((8, slots), F32),
                pltpu.VMEM((2 * ROWS[0], STEP), BF16),
                pltpu.VMEM((2 * ROWS[0], STEP), BF16),
                pltpu.VMEM((256, STEP), BF16),
                pltpu.VMEM((256, STEP), BF16),
                pltpu.VMEM((ROWS[0], 256), F32),
                pltpu.VMEM((384, 128), F32),
                pltpu.VMEM((128, 128), F32),
            ] + [pltpu.VMEM((Y_DEVS, 2 * KX, 128), F32) for _ in BLOCKS] * 2
            + [pltpu.VMEM((blocks * KX, 128), F32) for blocks in BLOCKS] + [
                pltpu.VMEM((Z_DEVS * EARLY * KX, 128), F32),
                pltpu.VMEM((Z_DEVS * LATE * KX, 128), F32),
                pltpu.VMEM((KX, 2 * KY, 256), F32),
                pltpu.VMEM((8, 128), F32),
                pltpu.VMEM((8, 8, 128), F32),
                pltpu.SemaphoreType.DMA((len(BLOCKS), 4)),
                pltpu.SemaphoreType.DMA((len(BLOCKS), 4)),
                pltpu.SemaphoreType.DMA((len(BLOCKS),)),
                pltpu.SemaphoreType.DMA((len(BLOCKS),)),
                pltpu.SemaphoreType.DMA((8,)),
                pltpu.SemaphoreType.DMA((8,)),
                pltpu.SemaphoreType.DMA((8,)),
                pltpu.SemaphoreType.DMA((SECTIONS, 4)),
            ],
            compiler_params=pltpu.CompilerParams(
                collective_id=0, has_side_effects=True, vmem_limit_bytes=60 * 1024 * 1024),
        )(charge.reshape(1, slots), real_mask.reshape(1, slots), grid_idx.T, jnp.transpose(spline_w, (1, 2, 0)),
          influence, *[jnp.asarray(table) for table in tables])
        return mode_energy, energy[0, 0:1]

    return jax.shard_map(local_energy, mesh=mesh, in_specs=(slot_spec, slot_spec, P(('sys', 'ydom', 'zdom'), None), P(('sys', 'ydom', 'zdom'), None, None), mode_spec), out_specs=(mode_spec, P('sys')), check_vma=False)
```

```python
import functools
import math
import jax
import jax.numpy as jnp
import numpy as np
from jax import lax
from jax.experimental import pallas as pl
from jax.experimental.pallas import tpu as pltpu
from jax.sharding import PartitionSpec as P

MESH = pl.DeviceIdType.MESH
F32 = jnp.float32
BF16 = jnp.bfloat16
G = 96
Y_DEVS = 4
Z_DEVS = 2
LEN_Y = 24
LEN_Z = 48
KX = 24
KY = 48
STEP = 2048
SPLIT = 1
UNROLL = 8
PART = 1024
PREP = 512
ROWS = (368, 368, 368, 336)
GHOST_ROW = (320, 320, 320, 288)
BLOCKS = (12, 12, 12, 3, 4, 4, 4)
WIDTH = (384, 384, 384, 128, 128, 128, 128)
GHOSTS = 3
LAST = (4, 5, 6)
SLOT = (0, 12, 24, 12, 0, 4, 8)
EARLY = 36
LATE = 16


def split_np(values):
    high = np.asarray(values, np.float32).astype(jnp.bfloat16)
    low = (np.asarray(values, np.float64) - high.astype(np.float64)).astype(jnp.bfloat16)
    return high, low


def dft_x():
    table = np.zeros((Y_DEVS, 2, KX, 128))
    for dest in range(Y_DEVS):
        angle = 2 * math.pi * (np.outer(np.arange(KX) + KX * dest, np.arange(G)) % G) / G
        table[dest, 0, :, :G] = np.cos(angle)
        table[dest, 1, :, :G] = -np.sin(angle)
    high, low = split_np(table.reshape(Y_DEVS * 2 * KX, 128))
    return np.concatenate([high, high], axis=1), low


def dft_y():
    table = np.zeros((2, Y_DEVS, 32, Z_DEVS, 128))
    for source in range(Y_DEVS):
        y_pos = LEN_Y * source + np.arange(LEN_Y + 3)
        for dest in range(Z_DEVS):
            angle = 2 * math.pi * (np.outer(y_pos, np.arange(KY) + KY * dest) % G) / G
            table[0, source, :LEN_Y + 3, dest, :KY] = np.cos(angle)
            table[1, source, :LEN_Y + 3, dest, :KY] = np.sin(angle)
            table[0, source, :LEN_Y + 3, dest, KY:2 * KY] = -np.sin(angle)
            table[1, source, :LEN_Y + 3, dest, KY:2 * KY] = np.cos(angle)
    return split_np(table.reshape(2 * Y_DEVS * 32, Z_DEVS * 128))


def dft_z(messages, slots):
    table = np.zeros((Z_DEVS, slots, 2, 128))
    for source in range(Z_DEVS):
        for message in messages:
            for block in range(BLOCKS[message]):
                if message == GHOSTS:
                    z_pos = LEN_Z + block
                elif message in LAST:
                    z_pos = 4 * (4 * (message - LAST[0]) + block) + 3
                else:
                    z_pos = 4 * block + message
                angle = 2 * math.pi * (((z_pos + LEN_Z * source) * np.arange(G)) % G) / G
                table[source, SLOT[message] + block, 0, :G] = np.cos(angle)
                table[source, SLOT[message] + block, 1, :G] = np.sin(angle)
    return split_np(table.reshape(Z_DEVS * slots, 256))


def split(values):
    high = values.astype(BF16)
    return high, (values - high.astype(F32)).astype(BF16)


def dot(lhs, rhs, lhs_dim, rhs_dim):
    return lax.dot_general(lhs, rhs, (((lhs_dim,), (rhs_dim,)), ((), ())), preferred_element_type=F32)


def kernel(charge, mask, grid_idx, spline_w, influence_in, fx2_in, fx_low_in, fy_high_in, fy_low_in, early_high_in,
           early_low_in, late_in, mode, energy_out,
           influence, fx2, fx_low, fy_high, fy_low, early_high, early_low, late,
           line_y, taps, base, lhs_a, lhs_b, rhs_a, rhs_b, total, packed, ghosts, *more):
    slots = charge.shape[1]
    me_y = lax.axis_index('ydom')
    me_z = lax.axis_index('zdom')
    me = me_z * Y_DEVS + me_y
    count = len(BLOCKS)
    sends, recvs, halves = more[:count], more[count:2 * count], more[2 * count:3 * count]
    (z_early, z_late, sums, part, parts,
     y_send_sem, y_recv_sem, z_send_sem, z_recv_sem, e_send_sem, e_recv_sem, in_sem) = more[3 * count:]

    loads = [pltpu.make_async_copy(source, dest, in_sem.at[index]) for index, (source, dest) in enumerate((
        (fx2_in, fx2), (fx_low_in, fx_low), (fy_high_in, fy_high), (fy_low_in, fy_low), (early_high_in, early_high),
        (early_low_in, early_low), (late_in, late), (influence_in, influence)))]
    for load in loads:
        load.start()

    def device(rank):
        return {'zdom': rank // Y_DEVS, 'ydom': rank % Y_DEVS}

    barrier = pltpu.get_barrier_semaphore()
    for shift in range(1, 8):
        pl.semaphore_signal(barrier, inc=1, device_id=device((me + shift) % 8), device_id_type=MESH)

    row4 = lax.broadcasted_iota(jnp.int32, (4, PREP), 0)
    row16 = lax.broadcasted_iota(jnp.int32, (16, PART), 0)
    row40 = lax.broadcasted_iota(jnp.int32, (40, PREP), 0)
    row40 = jnp.where(row40 < 32, row40, row40 % 4 + 24)
    row16_f = row16.astype(F32)

    def prepare(start):
        at = pl.ds(start, PREP)
        base_x, base_y, base_z = grid_idx[0:1, at], grid_idx[1:2, at], grid_idx[2:3, at]
        weight = charge[0:1, at] * mask[0:1, at].astype(F32)
        values = jnp.zeros((40, PREP), F32)
        for tap in range(4):
            values = jnp.where(row40 == base_y + tap, spline_w[1, tap:tap + 1, at], values)
        high = values.astype(BF16).astype(F32)
        for half, lines in ((0, high), (1, values - high)):
            for index, (top, bottom) in enumerate(((0, 1), (2, 0), (1, 2), (4, 4), (2, 3))):
                line_y[index, half, :, at] = jnp.concatenate(
                    [lines[8 * top:8 * top + 8], lines[8 * bottom:8 * bottom + 8]], axis=0).astype(BF16)
        tap = (row4 - base_z) & 3
        values = jnp.where(tap < 2, jnp.where(tap == 0, spline_w[2, 0:1, at], spline_w[2, 1:2, at]),
                           jnp.where(tap == 2, spline_w[2, 2:3, at], spline_w[2, 3:4, at]))
        base[0:4, at] = ((base_z + tap) >> 2).astype(F32)
        base[4:5, at] = base_x.astype(F32)
        weight_x = spline_w[0, :, at] * weight
        for chunk in range(4):
            product = weight_x * values[chunk:chunk + 1]
            high = product.astype(BF16).astype(F32)
            taps[chunk, 0:4, at] = high
            taps[chunk, 4:8, at] = product - high

    def build(chunk, start, to, lhs, rhs):
        at = pl.ds(start, PART)

        def spread_row(values):
            return jnp.broadcast_to(values, (16, PART)).astype(BF16)

        base_x = jnp.broadcast_to(base[4:5, at], (16, PART))
        rows = [spread_row(taps[chunk, index:index + 1, at]) for index in range(8)]
        zero = jnp.zeros((16, PART), BF16)
        offset = (row16_f - base_x).astype(BF16)
        wrapped = jnp.where(offset < jnp.asarray(-90, BF16), offset + jnp.asarray(G, BF16), offset)
        for group in range(G // 16):
            high, low = zero, zero
            for tap in range(4):
                hit = (offset if group else wrapped) == jnp.asarray(tap - 16 * group, BF16)
                high = jnp.where(hit, rows[tap], high)
                low = jnp.where(hit, rows[4 + tap], low)
            rhs[16 * group:16 * group + 16, to:to + PART] = high
            rhs[128 + 16 * group:144 + 16 * group, to:to + PART] = low
        block = jnp.broadcast_to(base[chunk:chunk + 1, at], (16, PART))
        block_a = block.astype(BF16)
        block_b = (block - (row16 // 8).astype(F32)).astype(BF16)
        block_g = (block - (row16 // 4).astype(F32)).astype(BF16)
        tiles = []
        for pair in range(6):
            tiles += [(block_a, 2 * pair, 0), (block_b, 2 * pair, 1), (block_a, 2 * pair + 1, 2)]
        if chunk < 3:
            tiles += [(block_a, 12, 0), (block_a, 12, 4)]
        tiles += [(block_g, 0, 3), (block_g, 4, 3), (block_g, 8, 3)]
        for index, (source, value, pattern) in enumerate(tiles):
            hit = source == jnp.asarray(value, BF16)
            for half in range(2):
                lhs[half * ROWS[chunk] + 16 * index:half * ROWS[chunk] + 16 * index + 16, to:to + PART] = jnp.where(
                    hit, line_y[pattern, half, :, at], zero)

    def spread(chunk, first, last):
        rows = ROWS[chunk]

        def fill(step, lhs, rhs):
            start = pl.multiple_of(jnp.minimum(step, slots // STEP - 1) * STEP, STEP)
            for to in range(0, STEP, PART):
                build(chunk, start + to, to, lhs, rhs)

        def add(lhs, rhs):
            product = dot(lhs[0:2 * rows, :], rhs[...], 1, 1)
            total[0:rows, :] += product[:rows] + product[rows:]

        if first == 0:
            total[...] = jnp.zeros_like(total)
            fill(0, lhs_a, rhs_a)

        def body(pair, carry):
            add(lhs_a, rhs_a)
            fill(2 * pair + 1, lhs_b, rhs_b)
            add(lhs_b, rhs_b)
            fill(2 * pair + 2, lhs_a, rhs_a)
            return carry

        lax.fori_loop(first, last, body, 0)

    row8 = lax.broadcasted_iota(jnp.int32, (8, 128), 0)

    def pack(chunk, first, last):
        def lines(start, rows):
            return total[start:start + rows, 0:128] + total[start:start + rows, 128:256]

        for pair in range(first, last):
            ghost = lines(GHOST_ROW[chunk] + 8 * pair, 8)
            packed[64 * pair:64 * pair + 24, :] = lines(48 * pair, 24)
            packed[64 * pair + 24:64 * pair + 32, :] = jnp.where(row8 < 4, ghost, 0.0)
            packed[64 * pair + 32:64 * pair + 56, :] = lines(48 * pair + 24, 24)
            packed[64 * pair + 56:64 * pair + 64, :] = jnp.where(row8 < 4, pltpu.roll(ghost, 4, 0), 0.0)
        if chunk < 3:
            ghosts[32 * chunk:32 * chunk + 32, :] = lines(288, 32)

    def transform_x(message, values):
        high, low = split(values)
        lines_k = dot(fx2[...], jnp.concatenate([high, low], axis=1), 1, 1) + dot(fx_low[...], high, 1, 1)
        for dest in range(Y_DEVS):
            sends[message][dest] = lines_k[48 * dest:48 * dest + 48]
        recvs[message][me_y] = sends[message][me_y]

    def copy_y(chunk, shift):
        dest = (me_y + shift) % Y_DEVS
        return pltpu.make_async_remote_copy(
            src_ref=sends[chunk].at[dest], dst_ref=recvs[chunk].at[me_y],
            send_sem=y_send_sem.at[chunk, shift], recv_sem=y_recv_sem.at[chunk, shift],
            device_id={'ydom': dest}, device_id_type=MESH)

    def start_y(chunk):
        for shift in (2, 1, 3):
            copy_y(chunk, shift).start()

    def wait_y(chunk):
        for shift in (2, 1, 3):
            copy_y(chunk, shift).wait()

    lane = lax.broadcasted_iota(jnp.int32, (KX, 128), 1)

    def regroup(blocks):
        out = list(blocks)
        for first, second in ((0, 2), (1, 3)):
            one, two = out[first], out[second]
            out[first] = jnp.where(lane < 64, one, pltpu.roll(two, 64, 1))
            out[second] = jnp.where(lane < 64, pltpu.roll(one, 64, 1), two)
        for first, second in ((0, 1), (2, 3)):
            one, two = out[first], out[second]
            even = (lane // 32) % 2 == 0
            out[first] = jnp.where(even, one, pltpu.roll(two, 32, 1))
            out[second] = jnp.where(even, pltpu.roll(one, 96, 1), two)
        return out

    def z_rows(message):
        per_source = EARLY if message < GHOSTS else LATE
        return pl.ds((me_z * per_source + SLOT[message]) * KX, BLOCKS[message] * KX)

    def z_buffer(message):
        return z_early if message < GHOSTS else z_late

    def copy_z(message):
        return pltpu.make_async_remote_copy(
            src_ref=halves[message], dst_ref=z_buffer(message).at[z_rows(message)],
            send_sem=z_send_sem.at[message], recv_sem=z_recv_sem.at[message],
            device_id={'zdom': 1 - me_z}, device_id_type=MESH)

    def transform_y(message):
        wait_y(message)
        recv = recvs[message]
        lines_re, lines_im = [], []
        for tile in range(WIDTH[message] // 128):
            for part_id, lines in ((0, lines_re), (1, lines_im)):
                lines += regroup([recv[source, KX * part_id:KX * part_id + KX, 128 * tile:128 * tile + 128]
                                  for source in range(Y_DEVS)])
        blocks = BLOCKS[message]
        values = jnp.concatenate([jnp.concatenate(lines_re[:blocks], axis=0), jnp.concatenate(lines_im[:blocks], axis=0)], axis=1)
        high, low = split(values)
        lines_k = dot(high, fy_high[...], 1, 0) + dot(high, fy_low[...], 1, 0) + dot(low, fy_high[...], 1, 0)
        first = me_z == 0
        halves[message][...] = jnp.where(first, lines_k[:, 128:], lines_k[:, :128])
        z_buffer(message)[z_rows(message), :] = jnp.where(first, lines_k[:, :128], lines_k[:, 128:])
        copy_z(message).start()

    rhs_a[...] = jnp.zeros_like(rhs_a)
    rhs_b[...] = jnp.zeros_like(rhs_b)
    ghosts[...] = jnp.zeros_like(ghosts)
    for source in range(Z_DEVS):
        z_late[((source + 1) * LATE - 1) * KX:(source + 1) * LATE * KX, :] = jnp.zeros((KX, 128), F32)

    def prepare_step(step, carry):
        prepare(pl.multiple_of(step * PREP, PREP))
        return carry

    lax.fori_loop(0, slots // PREP, prepare_step, 0)

    steps = slots // STEP // 2
    for chunk in range(3):
        spread(chunk, 0, steps)
        pack(chunk, 0, 6)
        if chunk == 0:
            for load in loads:
                load.wait()
        transform_x(chunk, packed[...])
        if chunk == 0:
            pl.semaphore_wait(barrier, 7)
        start_y(chunk)
        if chunk == 2:
            transform_x(GHOSTS, ghosts[...])
            start_y(GHOSTS)
        if chunk > 0:
            transform_y(chunk - 1)
    spread(3, 0, steps - SPLIT)
    transform_y(2)
    spread(3, steps - SPLIT, steps)
    for index, message in enumerate(LAST):
        pack(3, 2 * index, 2 * index + 2)
        transform_x(message, packed[128 * index:128 * index + 128, :])
        start_y(message)
    transform_y(GHOSTS)
    for message in range(3):
        copy_z(message).wait()
    def sum_early(index, carry):
        high, low = split(z_early[pl.ds(index, Z_DEVS * EARLY, stride=KX), :])
        high, low = high[:, :2 * KY], low[:, :2 * KY]
        sums[index] = dot(high, early_high[...], 0, 0) + dot(high, early_low[...], 0, 0) + dot(low, early_high[...], 0, 0)
        return carry

    lax.fori_loop(0, KX, sum_early, 0, unroll=UNROLL)
    for message in LAST:
        transform_y(message)
    for message in (GHOSTS,) + LAST:
        copy_z(message).wait()

    def sum_late(index, energy_sum):
        high, low = split(z_late[pl.ds(index, Z_DEVS * LATE, stride=KX), :])
        values = jnp.concatenate([high, low, high], axis=0)[:, :2 * KY]
        lines_k = sums[index] + dot(values, late[...], 0, 0)
        real = lines_k[0:KY, 0:G] + lines_k[KY:2 * KY, 128:128 + G]
        imag = lines_k[KY:2 * KY, 0:G] - lines_k[0:KY, 128:128 + G]
        energy = 0.5 * influence[index] * (real * real + imag * imag)
        mode[index] = energy
        return energy_sum + energy

    energy_sum = jnp.zeros((KY, G), F32)
    for index in range(3):
        energy_sum = lax.fori_loop(8 * index, 8 * index + 8, sum_late, energy_sum, unroll=UNROLL)
    part[...] = jnp.broadcast_to(jnp.sum(energy_sum), (8, 128))
    parts[me] = part[...]

    def copy_e(shift):
        return pltpu.make_async_remote_copy(
            src_ref=part, dst_ref=parts.at[me], send_sem=e_send_sem.at[shift], recv_sem=e_recv_sem.at[shift],
            device_id=device((me + shift) % 8), device_id_type=MESH)

    for shift in range(1, 8):
        copy_e(shift).start()
    for shift in range(1, 8):
        copy_e(shift).wait()
    result = parts[0]
    for rank in range(1, 8):
        result = result + parts[rank]
    energy_out[...] = result * (1.0 / (G * G * G))


def solution(mesh):
    slot_spec = P(('sys', 'ydom', 'zdom'))
    mode_spec = P(('sys', 'ydom'), 'zdom', None)
    late_high, late_low = dft_z((GHOSTS,) + LAST, LATE)
    tables = dft_x() + dft_y() + dft_z((0, 1, 2), EARLY) + (np.concatenate([late_high, late_high, late_low], axis=0),)

    def local_energy(charge, real_mask, grid_idx, spline_w, influence):
        slots = charge.shape[0]
        vmem = pl.BlockSpec(memory_space=pltpu.VMEM)
        whole = pl.BlockSpec(memory_space=pl.ANY)
        mode_energy, energy = pl.pallas_call(
            kernel,
            out_shape=(pltpu.VMEM((KX, KY, G), F32), pltpu.VMEM((8, 128), F32)),
            in_specs=[vmem] * 4 + [whole] * (1 + len(tables)),
            out_specs=(vmem, vmem),
            scratch_shapes=[
                pltpu.VMEM(influence.shape, F32),
            ] + [pltpu.VMEM(table.shape, BF16) for table in tables] + [
                pltpu.VMEM((5, 2, 16, slots), BF16),
                pltpu.VMEM((4, 8, slots), F32),
                pltpu.VMEM((8, slots), F32),
                pltpu.VMEM((2 * ROWS[0], STEP), BF16),
                pltpu.VMEM((2 * ROWS[0], STEP), BF16),
                pltpu.VMEM((256, STEP), BF16),
                pltpu.VMEM((256, STEP), BF16),
                pltpu.VMEM((ROWS[0], 256), F32),
                pltpu.VMEM((384, 128), F32),
                pltpu.VMEM((128, 128), F32),
            ] + [pltpu.VMEM((Y_DEVS, 2 * KX, width), F32) for width in WIDTH] * 2
            + [pltpu.VMEM((blocks * KX, 128), F32) for blocks in BLOCKS] + [
                pltpu.VMEM((Z_DEVS * EARLY * KX, 128), F32),
                pltpu.VMEM((Z_DEVS * LATE * KX, 128), F32),
                pltpu.VMEM((KX, 2 * KY, 256), F32),
                pltpu.VMEM((8, 128), F32),
                pltpu.VMEM((8, 8, 128), F32),
                pltpu.SemaphoreType.DMA((len(BLOCKS), 4)),
                pltpu.SemaphoreType.DMA((len(BLOCKS), 4)),
                pltpu.SemaphoreType.DMA((len(BLOCKS),)),
                pltpu.SemaphoreType.DMA((len(BLOCKS),)),
                pltpu.SemaphoreType.DMA((8,)),
                pltpu.SemaphoreType.DMA((8,)),
                pltpu.SemaphoreType.DMA((8,)),
            ],
            compiler_params=pltpu.CompilerParams(
                collective_id=0, has_side_effects=True, vmem_limit_bytes=60 * 1024 * 1024),
        )(charge.reshape(1, slots), real_mask.reshape(1, slots), grid_idx.T, jnp.transpose(spline_w, (1, 2, 0)),
          influence, *[jnp.asarray(table) for table in tables])
        return mode_energy, energy[0, 0:1]

    return jax.shard_map(local_energy, mesh=mesh, in_specs=(slot_spec, slot_spec, P(('sys', 'ydom', 'zdom'), None), P(('sys', 'ydom', 'zdom'), None, None), mode_spec), out_specs=(mode_spec, P('sys')), check_vma=False)
```

```python
import functools
import math
import jax
import jax.numpy as jnp
import numpy as np
from jax import lax
from jax.experimental import pallas as pl
from jax.experimental.pallas import tpu as pltpu
from jax.sharding import PartitionSpec as P

MESH = pl.DeviceIdType.MESH
F32 = jnp.float32
BF16 = jnp.bfloat16
G = 96
Y_DEVS = 4
Z_DEVS = 2
LEN_Y = 24
LEN_Z = 48
KX = 24
KY = 48
STEP = 2048
SPLIT = 1
UNROLL = 8
PART = 1024
PREP = 512
ROWS = (368, 368, 368, 336)
BLOCKS = (12, 12, 12, 3, 4, 4, 4)
WIDTH = (384, 384, 384, 128, 128, 128, 128)
GHOSTS = 3
LAST = (4, 5, 6)
SLOT = (0, 12, 24, 12, 0, 4, 8)
EARLY = 36
LATE = 16


def split_np(values):
    high = np.asarray(values, np.float32).astype(jnp.bfloat16)
    low = (np.asarray(values, np.float64) - high.astype(np.float64)).astype(jnp.bfloat16)
    return high, low


def dft_x():
    table = np.zeros((Y_DEVS, 2, KX, 128))
    for dest in range(Y_DEVS):
        angle = 2 * math.pi * (np.outer(np.arange(KX) + KX * dest, np.arange(G)) % G) / G
        table[dest, 0, :, :G] = np.cos(angle)
        table[dest, 1, :, :G] = -np.sin(angle)
    high, low = split_np(table.reshape(Y_DEVS * 2 * KX, 128))
    return np.concatenate([high, high], axis=1), low


def dft_y():
    table = np.zeros((2, Y_DEVS, 32, Z_DEVS, 128))
    for source in range(Y_DEVS):
        y_pos = LEN_Y * source + np.arange(LEN_Y + 3)
        for dest in range(Z_DEVS):
            angle = 2 * math.pi * (np.outer(y_pos, np.arange(KY) + KY * dest) % G) / G
            table[0, source, :LEN_Y + 3, dest, :KY] = np.cos(angle)
            table[1, source, :LEN_Y + 3, dest, :KY] = np.sin(angle)
            table[0, source, :LEN_Y + 3, dest, KY:2 * KY] = -np.sin(angle)
            table[1, source, :LEN_Y + 3, dest, KY:2 * KY] = np.cos(angle)
    return split_np(table.reshape(2 * Y_DEVS * 32, Z_DEVS * 128))


def dft_z(messages, slots):
    table = np.zeros((Z_DEVS, slots, 2, 128))
    for source in range(Z_DEVS):
        for message in messages:
            for block in range(BLOCKS[message]):
                if message == GHOSTS:
                    z_pos = LEN_Z + block
                elif message in LAST:
                    z_pos = 4 * (4 * (message - LAST[0]) + block) + 3
                else:
                    z_pos = 4 * block + message
                angle = 2 * math.pi * (((z_pos + LEN_Z * source) * np.arange(G)) % G) / G
                table[source, SLOT[message] + block, 0, :G] = np.cos(angle)
                table[source, SLOT[message] + block, 1, :G] = np.sin(angle)
    return split_np(table.reshape(Z_DEVS * slots, 256))


def split(values):
    high = values.astype(BF16)
    return high, (values - high.astype(F32)).astype(BF16)


def dot(lhs, rhs, lhs_dim, rhs_dim):
    return lax.dot_general(lhs, rhs, (((lhs_dim,), (rhs_dim,)), ((), ())), preferred_element_type=F32)


def kernel(charge, mask, grid_idx, spline_w, influence_in, fx2_in, fx_low_in, fy_high_in, fy_low_in, early_high_in,
           early_low_in, late_in, mode, energy_out,
           influence, fx2, fx_low, fy_high, fy_low, early_high, early_low, late,
           line_y, taps, base, lhs_a, lhs_b, rhs_a, rhs_b, total, packed, ghosts, *more):
    slots = charge.shape[1]
    me_y = lax.axis_index('ydom')
    me_z = lax.axis_index('zdom')
    me = me_z * Y_DEVS + me_y
    count = len(BLOCKS)
    sends, recvs, halves = more[:count], more[count:2 * count], more[2 * count:3 * count]
    (z_early, z_late, sums, part, parts,
     y_send_sem, y_recv_sem, z_send_sem, z_recv_sem, e_send_sem, e_recv_sem, in_sem) = more[3 * count:]

    loads = [pltpu.make_async_copy(source, dest, in_sem.at[index]) for index, (source, dest) in enumerate((
        (fx2_in, fx2), (fx_low_in, fx_low), (fy_high_in, fy_high), (fy_low_in, fy_low), (early_high_in, early_high),
        (early_low_in, early_low), (late_in, late), (influence_in, influence)))]
    for load in loads:
        load.start()

    def device(rank):
        return {'zdom': rank // Y_DEVS, 'ydom': rank % Y_DEVS}

    barrier = pltpu.get_barrier_semaphore()
    for shift in range(1, 8):
        pl.semaphore_signal(barrier, inc=1, device_id=device((me + shift) % 8), device_id_type=MESH)

    row4 = lax.broadcasted_iota(jnp.int32, (4, PREP), 0)
    row16 = lax.broadcasted_iota(jnp.int32, (16, PART), 0)
    row40 = lax.broadcasted_iota(jnp.int32, (40, PREP), 0)
    row40 = jnp.where(row40 < 32, row40, row40 % 4 + 24)
    row16_f = row16.astype(F32)

    def prepare(start):
        at = pl.ds(start, PREP)
        base_x, base_y, base_z = grid_idx[0:1, at], grid_idx[1:2, at], grid_idx[2:3, at]
        weight = charge[0:1, at] * mask[0:1, at].astype(F32)
        values = jnp.zeros((40, PREP), F32)
        for tap in range(4):
            values = jnp.where(row40 == base_y + tap, spline_w[1, tap:tap + 1, at], values)
        high = values.astype(BF16).astype(F32)
        for half, lines in ((0, high), (1, values - high)):
            for index, (top, bottom) in enumerate(((0, 1), (2, 0), (1, 2), (4, 4), (2, 3))):
                line_y[index, half, :, at] = jnp.concatenate(
                    [lines[8 * top:8 * top + 8], lines[8 * bottom:8 * bottom + 8]], axis=0).astype(BF16)
        tap = (row4 - base_z) & 3
        values = jnp.where(tap < 2, jnp.where(tap == 0, spline_w[2, 0:1, at], spline_w[2, 1:2, at]),
                           jnp.where(tap == 2, spline_w[2, 2:3, at], spline_w[2, 3:4, at]))
        block = ((base_z + tap) >> 2).astype(F32)
        base[:, at] = base_x.astype(F32)
        weight_x = spline_w[0, :, at] * weight
        for chunk in range(4):
            product = weight_x * values[chunk:chunk + 1]
            high = product.astype(BF16).astype(F32)
            taps[chunk, 0:4, at] = high
            taps[chunk, 4:8, at] = product - high
            taps[chunk, 8:9, at] = block[chunk:chunk + 1]

    def build(chunk, ghosts_too, start, to, lhs, rhs):
        at = pl.ds(start, PART)

        def spread_row(values):
            return jnp.broadcast_to(values, (16, PART)).astype(BF16)

        base_x = jnp.broadcast_to(base[:, at], (16, PART))
        rows = [spread_row(taps[chunk, index:index + 1, at]) for index in range(8)]
        zero = jnp.zeros((16, PART), BF16)
        offset = (row16_f - base_x).astype(BF16)
        wrapped = jnp.where(offset < jnp.asarray(-90, BF16), offset + jnp.asarray(G, BF16), offset)
        for group in range(G // 16):
            high, low = zero, zero
            for tap in range(4):
                hit = (offset if group else wrapped) == jnp.asarray(tap - 16 * group, BF16)
                high = jnp.where(hit, rows[tap], high)
                low = jnp.where(hit, rows[4 + tap], low)
            rhs[16 * group:16 * group + 16, to:to + PART] = high
            rhs[128 + 16 * group:144 + 16 * group, to:to + PART] = low
        block = jnp.broadcast_to(taps[chunk, 8:9, at], (16, PART))
        block_a = block.astype(BF16)
        block_b = (block - (row16 // 8).astype(F32)).astype(BF16)
        block_g = (block - (row16 // 4).astype(F32)).astype(BF16)
        tiles = []
        for pair in range(6):
            tiles += [(block_a, 2 * pair, 0), (block_b, 2 * pair, 1), (block_a, 2 * pair + 1, 2)]
        tiles += [(block_g, 0, 3), (block_g, 4, 3), (block_g, 8, 3)]
        if ghosts_too:
            tiles += [(block_a, 12, 0), (block_a, 12, 4)]
        for index, (source, value, pattern) in enumerate(tiles):
            hit = source == jnp.asarray(value, BF16)
            for half in range(2):
                lhs[half * ROWS[0] + 16 * index:half * ROWS[0] + 16 * index + 16, to:to + PART] = jnp.where(
                    hit, line_y[pattern, half, :, at], zero)

    def spread(chunk, first, last):
        rows = ROWS[chunk]

        count = slots // STEP

        def fill(step, lhs, rhs):
            ahead = step // count if chunk < 3 else 0
            start = pl.multiple_of((step % count) * STEP, STEP)
            for to in range(0, STEP, PART):
                build(chunk + ahead, chunk < 3, start + to, to, lhs, rhs)

        def add(lhs, rhs):
            product = dot(jnp.concatenate([lhs[0:rows, :], lhs[ROWS[0]:ROWS[0] + rows, :]], axis=0), rhs[...], 1, 1)
            total[0:rows, :] += product[:rows] + product[rows:]

        if first == 0:
            total[...] = jnp.zeros_like(total)
            if chunk == 0:
                fill(0, lhs_a, rhs_a)

        def body(pair, carry):
            add(lhs_a, rhs_a)
            fill(2 * pair + 1, lhs_b, rhs_b)
            add(lhs_b, rhs_b)
            fill(2 * pair + 2, lhs_a, rhs_a)
            return carry

        lax.fori_loop(first, last, body, 0)

    row8 = lax.broadcasted_iota(jnp.int32, (8, 128), 0)

    def pack(chunk, first, last):
        def lines(start, rows):
            return total[start:start + rows, 0:128] + total[start:start + rows, 128:256]

        for pair in range(first, last):
            ghost = lines(288 + 8 * pair, 8)
            packed[64 * pair:64 * pair + 24, :] = lines(48 * pair, 24)
            packed[64 * pair + 24:64 * pair + 32, :] = jnp.where(row8 < 4, ghost, 0.0)
            packed[64 * pair + 32:64 * pair + 56, :] = lines(48 * pair + 24, 24)
            packed[64 * pair + 56:64 * pair + 64, :] = jnp.where(row8 < 4, pltpu.roll(ghost, 4, 0), 0.0)
        if chunk < 3:
            ghosts[32 * chunk:32 * chunk + 32, :] = lines(336, 32)

    def transform_x(message, values):
        high, low = split(values)
        lines_k = dot(fx2[...], jnp.concatenate([high, low], axis=1), 1, 1) + dot(fx_low[...], high, 1, 1)
        for dest in range(Y_DEVS):
            sends[message][dest] = lines_k[48 * dest:48 * dest + 48]
        recvs[message][me_y] = sends[message][me_y]

    def copy_y(chunk, shift):
        dest = (me_y + shift) % Y_DEVS
        return pltpu.make_async_remote_copy(
            src_ref=sends[chunk].at[dest], dst_ref=recvs[chunk].at[me_y],
            send_sem=y_send_sem.at[chunk, shift], recv_sem=y_recv_sem.at[chunk, shift],
            device_id={'ydom': dest}, device_id_type=MESH)

    def start_y(chunk):
        for shift in (2, 1, 3):
            copy_y(chunk, shift).start()

    def wait_y(chunk):
        for shift in (2, 1, 3):
            copy_y(chunk, shift).wait()

    lane = lax.broadcasted_iota(jnp.int32, (KX, 128), 1)

    def regroup(blocks):
        out = list(blocks)
        for first, second in ((0, 2), (1, 3)):
            one, two = out[first], out[second]
            out[first] = jnp.where(lane < 64, one, pltpu.roll(two, 64, 1))
            out[second] = jnp.where(lane < 64, pltpu.roll(one, 64, 1), two)
        for first, second in ((0, 1), (2, 3)):
            one, two = out[first], out[second]
            even = (lane // 32) % 2 == 0
            out[first] = jnp.where(even, one, pltpu.roll(two, 32, 1))
            out[second] = jnp.where(even, pltpu.roll(one, 96, 1), two)
        return out

    def z_rows(message):
        per_source = EARLY if message < GHOSTS else LATE
        return pl.ds((me_z * per_source + SLOT[message]) * KX, BLOCKS[message] * KX)

    def z_buffer(message):
        return z_early if message < GHOSTS else z_late

    def copy_z(message):
        return pltpu.make_async_remote_copy(
            src_ref=halves[message], dst_ref=z_buffer(message).at[z_rows(message)],
            send_sem=z_send_sem.at[message], recv_sem=z_recv_sem.at[message],
            device_id={'zdom': 1 - me_z}, device_id_type=MESH)

    def transform_y(message):
        recv = recvs[message]
        lines_re, lines_im = [], []
        for tile in range(WIDTH[message] // 128):
            for part_id, lines in ((0, lines_re), (1, lines_im)):
                lines += regroup([recv[source, KX * part_id:KX * part_id + KX, 128 * tile:128 * tile + 128]
                                  for source in range(Y_DEVS)])
        blocks = BLOCKS[message]
        values = jnp.concatenate([jnp.concatenate(lines_re[:blocks], axis=0), jnp.concatenate(lines_im[:blocks], axis=0)], axis=1)
        high, low = split(values)
        lines_k = dot(high, fy_high[...], 1, 0) + dot(high, fy_low[...], 1, 0) + dot(low, fy_high[...], 1, 0)
        first = me_z == 0
        halves[message][...] = jnp.where(first, lines_k[:, 128:], lines_k[:, :128])
        z_buffer(message)[z_rows(message), :] = jnp.where(first, lines_k[:, :128], lines_k[:, 128:])

    for rhs in (rhs_a, rhs_b):
        for row in (G, 128 + G):
            rhs[row:row + 32, :] = jnp.zeros((32, STEP), BF16)
    ghosts[...] = jnp.zeros_like(ghosts)
    for source in range(Z_DEVS):
        z_late[((source + 1) * LATE - 1) * KX:(source + 1) * LATE * KX, :] = jnp.zeros((KX, 128), F32)

    def prepare_step(step, carry):
        prepare(pl.multiple_of(step * PREP, PREP))
        return carry

    lax.fori_loop(0, slots // PREP, prepare_step, 0)

    steps = slots // STEP // 2
    for chunk in range(3):
        spread(chunk, 0, steps)
        if chunk == 0:
            for load in loads:
                load.wait()
            pl.semaphore_wait(barrier, 7)
        else:
            wait_y(chunk - 1)
        pack(chunk, 0, 6)
        transform_x(chunk, packed[...])
        if chunk == 2:
            transform_x(GHOSTS, ghosts[...])
        if chunk > 0:
            transform_y(chunk - 1)
        start_y(chunk)
        if chunk == 2:
            start_y(GHOSTS)
        if chunk > 0:
            copy_z(chunk - 1).start()
    spread(3, 0, steps - SPLIT)
    wait_y(2)
    transform_y(2)
    copy_z(2).start()
    spread(3, steps - SPLIT, steps)
    for index, message in enumerate(LAST):
        pack(3, 2 * index, 2 * index + 2)
        transform_x(message, packed[128 * index:128 * index + 128, :])
        start_y(message)
    wait_y(GHOSTS)
    transform_y(GHOSTS)
    copy_z(GHOSTS).start()
    for message in range(3):
        copy_z(message).wait()
    def sum_early(index, carry):
        high, low = split(z_early[pl.ds(index, Z_DEVS * EARLY, stride=KX), :])
        high, low = high[:, :2 * KY], low[:, :2 * KY]
        sums[index] = dot(high, early_high[...], 0, 0) + dot(high, early_low[...], 0, 0) + dot(low, early_high[...], 0, 0)
        return carry

    lax.fori_loop(0, KX, sum_early, 0, unroll=UNROLL)
    for message in LAST:
        wait_y(message)
        transform_y(message)
        copy_z(message).start()
    for message in (GHOSTS,) + LAST:
        copy_z(message).wait()

    def sum_late(index, energy_sum):
        high, low = split(z_late[pl.ds(index, Z_DEVS * LATE, stride=KX), :])
        values = jnp.concatenate([high, low, high], axis=0)[:, :2 * KY]
        lines_k = sums[index] + dot(values, late[...], 0, 0)
        real = lines_k[0:KY, 0:G] + lines_k[KY:2 * KY, 128:128 + G]
        imag = lines_k[KY:2 * KY, 0:G] - lines_k[0:KY, 128:128 + G]
        energy = 0.5 * influence[index] * (real * real + imag * imag)
        mode[index] = energy
        return energy_sum + energy

    energy_sum = jnp.zeros((KY, G), F32)
    for index in range(3):
        energy_sum = lax.fori_loop(8 * index, 8 * index + 8, sum_late, energy_sum, unroll=UNROLL)
    part[...] = jnp.broadcast_to(jnp.sum(energy_sum), (8, 128))
    parts[me] = part[...]

    def copy_e(shift):
        return pltpu.make_async_remote_copy(
            src_ref=part, dst_ref=parts.at[me], send_sem=e_send_sem.at[shift], recv_sem=e_recv_sem.at[shift],
            device_id=device((me + shift) % 8), device_id_type=MESH)

    for shift in range(1, 8):
        copy_e(shift).start()
    for shift in range(1, 8):
        copy_e(shift).wait()
    result = parts[0]
    for rank in range(1, 8):
        result = result + parts[rank]
    energy_out[...] = result * (1.0 / (G * G * G))


def solution(mesh):
    slot_spec = P(('sys', 'ydom', 'zdom'))
    mode_spec = P(('sys', 'ydom'), 'zdom', None)
    late_high, late_low = dft_z((GHOSTS,) + LAST, LATE)
    tables = dft_x() + dft_y() + dft_z((0, 1, 2), EARLY) + (np.concatenate([late_high, late_high, late_low], axis=0),)

    def local_energy(charge, real_mask, grid_idx, spline_w, influence):
        slots = charge.shape[0]
        vmem = pl.BlockSpec(memory_space=pltpu.VMEM)
        whole = pl.BlockSpec(memory_space=pl.ANY)
        mode_energy, energy = pl.pallas_call(
            kernel,
            out_shape=(pltpu.VMEM((KX, KY, G), F32), pltpu.VMEM((8, 128), F32)),
            in_specs=[vmem] * 4 + [whole] * (1 + len(tables)),
            out_specs=(vmem, vmem),
            scratch_shapes=[
                pltpu.VMEM(influence.shape, F32),
            ] + [pltpu.VMEM(table.shape, BF16) for table in tables] + [
                pltpu.VMEM((5, 2, 16, slots), BF16),
                pltpu.VMEM((4, 9, slots), F32),
                pltpu.VMEM((1, slots), F32),
                pltpu.VMEM((2 * ROWS[0], STEP), BF16),
                pltpu.VMEM((2 * ROWS[0], STEP), BF16),
                pltpu.VMEM((256, STEP), BF16),
                pltpu.VMEM((256, STEP), BF16),
                pltpu.VMEM((ROWS[0], 256), F32),
                pltpu.VMEM((384, 128), F32),
                pltpu.VMEM((128, 128), F32),
            ] + [pltpu.VMEM((Y_DEVS, 2 * KX, width), F32) for width in WIDTH] * 2
            + [pltpu.VMEM((blocks * KX, 128), F32) for blocks in BLOCKS] + [
                pltpu.VMEM((Z_DEVS * EARLY * KX, 128), F32),
                pltpu.VMEM((Z_DEVS * LATE * KX, 128), F32),
                pltpu.VMEM((KX, 2 * KY, 256), F32),
                pltpu.VMEM((8, 128), F32),
                pltpu.VMEM((8, 8, 128), F32),
                pltpu.SemaphoreType.DMA((len(BLOCKS), 4)),
                pltpu.SemaphoreType.DMA((len(BLOCKS), 4)),
                pltpu.SemaphoreType.DMA((len(BLOCKS),)),
                pltpu.SemaphoreType.DMA((len(BLOCKS),)),
                pltpu.SemaphoreType.DMA((8,)),
                pltpu.SemaphoreType.DMA((8,)),
                pltpu.SemaphoreType.DMA((8,)),
            ],
            compiler_params=pltpu.CompilerParams(
                collective_id=0, has_side_effects=True, vmem_limit_bytes=60 * 1024 * 1024),
        )(charge.reshape(1, slots), real_mask.reshape(1, slots), grid_idx.T, jnp.transpose(spline_w, (1, 2, 0)),
          influence, *[jnp.asarray(table) for table in tables])
        return mode_energy, energy[0, 0:1]

    return jax.shard_map(local_energy, mesh=mesh, in_specs=(slot_spec, slot_spec, P(('sys', 'ydom', 'zdom'), None), P(('sys', 'ydom', 'zdom'), None, None), mode_spec), out_specs=(mode_spec, P('sys')), check_vma=False)
```

```python
import functools
import math
import jax
import jax.numpy as jnp
import numpy as np
from jax import lax
from jax.experimental import pallas as pl
from jax.experimental.pallas import tpu as pltpu
from jax.sharding import PartitionSpec as P

MESH = pl.DeviceIdType.MESH
F32 = jnp.float32
BF16 = jnp.bfloat16
G = 96
Y_DEVS = 4
Z_DEVS = 2
LEN_Y = 24
LEN_Z = 48
KX = 24
KY = 48
STEP = 2048
SPLIT = 1
UNROLL = 6
PART = 1024
PREP = 512
ROWS = (368, 368, 368, 336)
BLOCKS = (12, 12, 12, 3, 4, 4, 4)
WIDTH = (384, 384, 384, 128, 128, 128, 128)
GHOSTS = 3
LAST = (4, 5, 6)
SLOT = (0, 12, 24, 12, 0, 4, 8)
EARLY = 36
LATE = 16


def split_np(values):
    high = np.asarray(values, np.float32).astype(jnp.bfloat16)
    low = (np.asarray(values, np.float64) - high.astype(np.float64)).astype(jnp.bfloat16)
    return high, low


def dft_x():
    table = np.zeros((Y_DEVS, 2, KX, 128))
    for dest in range(Y_DEVS):
        angle = 2 * math.pi * (np.outer(np.arange(KX) + KX * dest, np.arange(G)) % G) / G
        table[dest, 0, :, :G] = np.cos(angle)
        table[dest, 1, :, :G] = -np.sin(angle)
    high, low = split_np(table.reshape(Y_DEVS * 2 * KX, 128))
    return np.concatenate([high, high], axis=1), low


def dft_y():
    table = np.zeros((2, Y_DEVS, 32, Z_DEVS, 128))
    for source in range(Y_DEVS):
        y_pos = LEN_Y * source + np.arange(LEN_Y + 3)
        for dest in range(Z_DEVS):
            angle = 2 * math.pi * (np.outer(y_pos, np.arange(KY) + KY * dest) % G) / G
            table[0, source, :LEN_Y + 3, dest, :KY] = np.cos(angle)
            table[1, source, :LEN_Y + 3, dest, :KY] = np.sin(angle)
            table[0, source, :LEN_Y + 3, dest, KY:2 * KY] = -np.sin(angle)
            table[1, source, :LEN_Y + 3, dest, KY:2 * KY] = np.cos(angle)
    return split_np(table.reshape(2 * Y_DEVS * 32, Z_DEVS * 128))


def dft_z(messages, slots):
    table = np.zeros((Z_DEVS, slots, 2, 128))
    for source in range(Z_DEVS):
        for message in messages:
            for block in range(BLOCKS[message]):
                if message == GHOSTS:
                    z_pos = LEN_Z + block
                elif message in LAST:
                    z_pos = 4 * (4 * (message - LAST[0]) + block) + 3
                else:
                    z_pos = 4 * block + message
                angle = 2 * math.pi * (((z_pos + LEN_Z * source) * np.arange(G)) % G) / G
                table[source, SLOT[message] + block, 0, :G] = np.cos(angle)
                table[source, SLOT[message] + block, 1, :G] = np.sin(angle)
    return split_np(table.reshape(Z_DEVS * slots, 256))


def split(values):
    high = values.astype(BF16)
    return high, (values - high.astype(F32)).astype(BF16)


def dot(lhs, rhs, lhs_dim, rhs_dim):
    return lax.dot_general(lhs, rhs, (((lhs_dim,), (rhs_dim,)), ((), ())), preferred_element_type=F32)


def kernel(charge, mask, grid_idx, spline_w, influence_in, fx2_in, fx_low_in, fy_high_in, fy_low_in, early_high_in,
           early_low_in, late_in, mode, energy_out,
           influence, fx2, fx_low, fy_high, fy_low, early_high, early_low, late,
           line_y, taps, base, lhs_a, lhs_b, rhs_a, rhs_b, total, packed, ghosts, *more):
    slots = charge.shape[1]
    me_y = lax.axis_index('ydom')
    me_z = lax.axis_index('zdom')
    me = me_z * Y_DEVS + me_y
    count = len(BLOCKS)
    sends, recvs, halves = more[:count], more[count:2 * count], more[2 * count:3 * count]
    (z_early, z_late, sums, part, parts,
     y_send_sem, y_recv_sem, z_send_sem, z_recv_sem, e_send_sem, e_recv_sem, in_sem) = more[3 * count:]

    loads = [pltpu.make_async_copy(source, dest, in_sem.at[index]) for index, (source, dest) in enumerate((
        (fx2_in, fx2), (fx_low_in, fx_low), (fy_high_in, fy_high), (fy_low_in, fy_low), (early_high_in, early_high),
        (early_low_in, early_low), (late_in, late), (influence_in, influence)))]
    for load in loads:
        load.start()

    def device(rank):
        return {'zdom': rank // Y_DEVS, 'ydom': rank % Y_DEVS}

    barrier = pltpu.get_barrier_semaphore()
    for shift in range(1, 8):
        pl.semaphore_signal(barrier, inc=1, device_id=device((me + shift) % 8), device_id_type=MESH)

    row4 = lax.broadcasted_iota(jnp.int32, (4, PREP), 0)
    row16 = lax.broadcasted_iota(jnp.int32, (16, PART), 0)
    row40 = lax.broadcasted_iota(jnp.int32, (40, PREP), 0)
    row40 = jnp.where(row40 < 32, row40, row40 % 4 + 24)
    row16_f = row16.astype(F32)

    def prepare(start):
        at = pl.ds(start, PREP)
        base_x, base_y, base_z = grid_idx[0:1, at], grid_idx[1:2, at], grid_idx[2:3, at]
        weight = charge[0:1, at] * mask[0:1, at].astype(F32)
        values = jnp.zeros((40, PREP), F32)
        for tap in range(4):
            values = jnp.where(row40 == base_y + tap, spline_w[1, tap:tap + 1, at], values)
        high = values.astype(BF16).astype(F32)
        for half, lines in ((0, high), (1, values - high)):
            for index, (top, bottom) in enumerate(((0, 1), (2, 0), (1, 2), (4, 4), (2, 3))):
                line_y[index, half, :, at] = jnp.concatenate(
                    [lines[8 * top:8 * top + 8], lines[8 * bottom:8 * bottom + 8]], axis=0).astype(BF16)
        tap = (row4 - base_z) & 3
        values = jnp.where(tap < 2, jnp.where(tap == 0, spline_w[2, 0:1, at], spline_w[2, 1:2, at]),
                           jnp.where(tap == 2, spline_w[2, 2:3, at], spline_w[2, 3:4, at]))
        block = ((base_z + tap) >> 2).astype(F32)
        base[:, at] = base_x.astype(F32)
        weight_x = spline_w[0, :, at] * weight
        for chunk in range(4):
            product = weight_x * values[chunk:chunk + 1]
            high = product.astype(BF16).astype(F32)
            taps[chunk, 0:4, at] = high
            taps[chunk, 4:8, at] = product - high
            taps[chunk, 8:9, at] = block[chunk:chunk + 1]

    def build(chunk, ghosts_too, start, to, lhs, rhs):
        at = pl.ds(start, PART)

        def spread_row(values):
            return jnp.broadcast_to(values, (16, PART)).astype(BF16)

        base_x = jnp.broadcast_to(base[:, at], (16, PART))
        rows = [spread_row(taps[chunk, index:index + 1, at]) for index in range(8)]
        zero = jnp.zeros((16, PART), BF16)
        offset = (row16_f - base_x).astype(BF16)
        wrapped = jnp.where(offset < jnp.asarray(-90, BF16), offset + jnp.asarray(G, BF16), offset)
        for group in range(G // 16):
            high, low = zero, zero
            for tap in range(4):
                hit = (offset if group else wrapped) == jnp.asarray(tap - 16 * group, BF16)
                high = jnp.where(hit, rows[tap], high)
                low = jnp.where(hit, rows[4 + tap], low)
            rhs[16 * group:16 * group + 16, to:to + PART] = high
            rhs[128 + 16 * group:144 + 16 * group, to:to + PART] = low
        block = jnp.broadcast_to(taps[chunk, 8:9, at], (16, PART))
        block_a = block.astype(BF16)
        block_b = (block - (row16 // 8).astype(F32)).astype(BF16)
        block_g = (block - (row16 // 4).astype(F32)).astype(BF16)
        tiles = []
        for pair in range(6):
            tiles += [(block_a, 2 * pair, 0), (block_b, 2 * pair, 1), (block_a, 2 * pair + 1, 2)]
        tiles += [(block_g, 0, 3), (block_g, 4, 3), (block_g, 8, 3)]
        if ghosts_too:
            tiles += [(block_a, 12, 0), (block_a, 12, 4)]
        for index, (source, value, pattern) in enumerate(tiles):
            hit = source == jnp.asarray(value, BF16)
            for half in range(2):
                lhs[half * ROWS[0] + 16 * index:half * ROWS[0] + 16 * index + 16, to:to + PART] = jnp.where(
                    hit, line_y[pattern, half, :, at], zero)

    def spread(chunk, first, last):
        rows = ROWS[chunk]

        count = slots // STEP

        def fill(step, lhs, rhs):
            ahead = step // count if chunk < 3 else 0
            start = pl.multiple_of((step % count) * STEP, STEP)
            for to in range(0, STEP, PART):
                build(chunk + ahead, chunk < 3, start + to, to, lhs, rhs)

        def add(lhs, rhs):
            product = dot(jnp.concatenate([lhs[0:rows, :], lhs[ROWS[0]:ROWS[0] + rows, :]], axis=0), rhs[...], 1, 1)
            total[0:rows, :] += product[:rows] + product[rows:]

        if first == 0:
            total[...] = jnp.zeros_like(total)
            if chunk == 0:
                fill(0, lhs_a, rhs_a)

        def body(pair, carry):
            add(lhs_a, rhs_a)
            fill(2 * pair + 1, lhs_b, rhs_b)
            add(lhs_b, rhs_b)
            fill(2 * pair + 2, lhs_a, rhs_a)
            return carry

        lax.fori_loop(first, last, body, 0)

    row8 = lax.broadcasted_iota(jnp.int32, (8, 128), 0)

    def pack(chunk, first, last):
        def lines(start, rows):
            return total[start:start + rows, 0:128] + total[start:start + rows, 128:256]

        for pair in range(first, last):
            ghost = lines(288 + 8 * pair, 8)
            packed[64 * pair:64 * pair + 24, :] = lines(48 * pair, 24)
            packed[64 * pair + 24:64 * pair + 32, :] = jnp.where(row8 < 4, ghost, 0.0)
            packed[64 * pair + 32:64 * pair + 56, :] = lines(48 * pair + 24, 24)
            packed[64 * pair + 56:64 * pair + 64, :] = jnp.where(row8 < 4, pltpu.roll(ghost, 4, 0), 0.0)
        if chunk < 3:
            ghosts[32 * chunk:32 * chunk + 32, :] = lines(336, 32)

    def transform_x(message, values):
        high, low = split(values)
        lines_k = dot(fx2[...], jnp.concatenate([high, low], axis=1), 1, 1) + dot(fx_low[...], high, 1, 1)
        for dest in range(Y_DEVS):
            sends[message][dest] = lines_k[48 * dest:48 * dest + 48]
        recvs[message][me_y] = sends[message][me_y]

    def copy_y(chunk, shift):
        dest = (me_y + shift) % Y_DEVS
        return pltpu.make_async_remote_copy(
            src_ref=sends[chunk].at[dest], dst_ref=recvs[chunk].at[me_y],
            send_sem=y_send_sem.at[chunk, shift], recv_sem=y_recv_sem.at[chunk, shift],
            device_id={'ydom': dest}, device_id_type=MESH)

    def start_y(chunk):
        for shift in (2, 1, 3):
            copy_y(chunk, shift).start()

    def wait_y(chunk):
        for shift in (2, 1, 3):
            copy_y(chunk, shift).wait()

    lane = lax.broadcasted_iota(jnp.int32, (KX, 128), 1)

    def regroup(blocks):
        out = list(blocks)
        for first, second in ((0, 2), (1, 3)):
            one, two = out[first], out[second]
            out[first] = jnp.where(lane < 64, one, pltpu.roll(two, 64, 1))
            out[second] = jnp.where(lane < 64, pltpu.roll(one, 64, 1), two)
        for first, second in ((0, 1), (2, 3)):
            one, two = out[first], out[second]
            even = (lane // 32) % 2 == 0
            out[first] = jnp.where(even, one, pltpu.roll(two, 32, 1))
            out[second] = jnp.where(even, pltpu.roll(one, 96, 1), two)
        return out

    def z_rows(message):
        per_source = EARLY if message < GHOSTS else LATE
        return pl.ds((me_z * per_source + SLOT[message]) * KX, BLOCKS[message] * KX)

    def z_buffer(message):
        return z_early if message < GHOSTS else z_late

    def copy_z(message):
        return pltpu.make_async_remote_copy(
            src_ref=halves[message], dst_ref=z_buffer(message).at[z_rows(message)],
            send_sem=z_send_sem.at[message], recv_sem=z_recv_sem.at[message],
            device_id={'zdom': 1 - me_z}, device_id_type=MESH)

    def transform_y(message):
        recv = recvs[message]
        lines_re, lines_im = [], []
        for tile in range(WIDTH[message] // 128):
            for part_id, lines in ((0, lines_re), (1, lines_im)):
                lines += regroup([recv[source, KX * part_id:KX * part_id + KX, 128 * tile:128 * tile + 128]
                                  for source in range(Y_DEVS)])
        blocks = BLOCKS[message]
        values = jnp.concatenate([jnp.concatenate(lines_re[:blocks], axis=0), jnp.concatenate(lines_im[:blocks], axis=0)], axis=1)
        high, low = split(values)
        lines_k = dot(high, fy_high[...], 1, 0) + dot(high, fy_low[...], 1, 0) + dot(low, fy_high[...], 1, 0)
        first = me_z == 0
        halves[message][...] = jnp.where(first, lines_k[:, 128:], lines_k[:, :128])
        z_buffer(message)[z_rows(message), :] = jnp.where(first, lines_k[:, :128], lines_k[:, 128:])

    for rhs in (rhs_a, rhs_b):
        for row in (G, 128 + G):
            rhs[row:row + 32, :] = jnp.zeros((32, STEP), BF16)
    ghosts[...] = jnp.zeros_like(ghosts)
    for source in range(Z_DEVS):
        z_late[((source + 1) * LATE - 1) * KX:(source + 1) * LATE * KX, :] = jnp.zeros((KX, 128), F32)

    def prepare_step(step, carry):
        prepare(pl.multiple_of(step * PREP, PREP))
        return carry

    lax.fori_loop(0, slots // PREP, prepare_step, 0)

    steps = slots // STEP // 2
    for chunk in range(3):
        spread(chunk, 0, steps)
        if chunk == 0:
            for load in loads:
                load.wait()
            pl.semaphore_wait(barrier, 7)
        else:
            wait_y(chunk - 1)
        pack(chunk, 0, 6)
        transform_x(chunk, packed[...])
        if chunk == 2:
            transform_x(GHOSTS, ghosts[...])
        if chunk > 0:
            transform_y(chunk - 1)
        start_y(chunk)
        if chunk == 2:
            start_y(GHOSTS)
        if chunk > 0:
            copy_z(chunk - 1).start()
    spread(3, 0, steps - SPLIT)
    wait_y(2)
    transform_y(2)
    copy_z(2).start()
    spread(3, steps - SPLIT, steps)
    for index, message in enumerate(LAST):
        pack(3, 2 * index, 2 * index + 2)
        transform_x(message, packed[128 * index:128 * index + 128, :])
        start_y(message)
    wait_y(GHOSTS)
    transform_y(GHOSTS)
    copy_z(GHOSTS).start()
    def sum_early(index, carry):
        high, low = split(z_early[pl.ds(index, Z_DEVS * EARLY, stride=KX), :])
        high, low = high[:, :2 * KY], low[:, :2 * KY]
        sums[index] = dot(high, early_high[...], 0, 0) + dot(high, early_low[...], 0, 0) + dot(low, early_high[...], 0, 0)
        return carry

    for index, message in enumerate(LAST):
        wait_y(message)
        transform_y(message)
        copy_z(message).start()
        if index == 0:
            for early in range(3):
                copy_z(early).wait()
            lax.fori_loop(0, KX // 2, sum_early, 0, unroll=UNROLL)
        elif index == 1:
            lax.fori_loop(KX // 2, KX, sum_early, 0, unroll=UNROLL)
    for message in (GHOSTS,) + LAST:
        copy_z(message).wait()

    def sum_late(index, energy_sum):
        high, low = split(z_late[pl.ds(index, Z_DEVS * LATE, stride=KX), :])
        values = jnp.concatenate([high, low, high], axis=0)[:, :2 * KY]
        lines_k = sums[index] + dot(values, late[...], 0, 0)
        real = lines_k[0:KY, 0:G] + lines_k[KY:2 * KY, 128:128 + G]
        imag = lines_k[KY:2 * KY, 0:G] - lines_k[0:KY, 128:128 + G]
        energy = 0.5 * influence[index] * (real * real + imag * imag)
        mode[index] = energy
        return energy_sum + energy

    energy_sum = jnp.zeros((KY, G), F32)
    for index in range(3):
        energy_sum = lax.fori_loop(8 * index, 8 * index + 8, sum_late, energy_sum, unroll=8)
    part[...] = jnp.broadcast_to(jnp.sum(energy_sum), (8, 128))
    parts[me] = part[...]

    def copy_e(shift):
        return pltpu.make_async_remote_copy(
            src_ref=part, dst_ref=parts.at[me], send_sem=e_send_sem.at[shift], recv_sem=e_recv_sem.at[shift],
            device_id=device((me + shift) % 8), device_id_type=MESH)

    for shift in range(1, 8):
        copy_e(shift).start()
    for shift in range(1, 8):
        copy_e(shift).wait()
    result = parts[0]
    for rank in range(1, 8):
        result = result + parts[rank]
    energy_out[...] = result * (1.0 / (G * G * G))


def solution(mesh):
    slot_spec = P(('sys', 'ydom', 'zdom'))
    mode_spec = P(('sys', 'ydom'), 'zdom', None)
    late_high, late_low = dft_z((GHOSTS,) + LAST, LATE)
    tables = dft_x() + dft_y() + dft_z((0, 1, 2), EARLY) + (np.concatenate([late_high, late_high, late_low], axis=0),)

    def local_energy(charge, real_mask, grid_idx, spline_w, influence):
        slots = charge.shape[0]
        vmem = pl.BlockSpec(memory_space=pltpu.VMEM)
        whole = pl.BlockSpec(memory_space=pl.ANY)
        mode_energy, energy = pl.pallas_call(
            kernel,
            out_shape=(pltpu.VMEM((KX, KY, G), F32), pltpu.VMEM((8, 128), F32)),
            in_specs=[vmem] * 4 + [whole] * (1 + len(tables)),
            out_specs=(vmem, vmem),
            scratch_shapes=[
                pltpu.VMEM(influence.shape, F32),
            ] + [pltpu.VMEM(table.shape, BF16) for table in tables] + [
                pltpu.VMEM((5, 2, 16, slots), BF16),
                pltpu.VMEM((4, 9, slots), F32),
                pltpu.VMEM((1, slots), F32),
                pltpu.VMEM((2 * ROWS[0], STEP), BF16),
                pltpu.VMEM((2 * ROWS[0], STEP), BF16),
                pltpu.VMEM((256, STEP), BF16),
                pltpu.VMEM((256, STEP), BF16),
                pltpu.VMEM((ROWS[0], 256), F32),
                pltpu.VMEM((384, 128), F32),
                pltpu.VMEM((128, 128), F32),
            ] + [pltpu.VMEM((Y_DEVS, 2 * KX, width), F32) for width in WIDTH] * 2
            + [pltpu.VMEM((blocks * KX, 128), F32) for blocks in BLOCKS] + [
                pltpu.VMEM((Z_DEVS * EARLY * KX, 128), F32),
                pltpu.VMEM((Z_DEVS * LATE * KX, 128), F32),
                pltpu.VMEM((KX, 2 * KY, 256), F32),
                pltpu.VMEM((8, 128), F32),
                pltpu.VMEM((8, 8, 128), F32),
                pltpu.SemaphoreType.DMA((len(BLOCKS), 4)),
                pltpu.SemaphoreType.DMA((len(BLOCKS), 4)),
                pltpu.SemaphoreType.DMA((len(BLOCKS),)),
                pltpu.SemaphoreType.DMA((len(BLOCKS),)),
                pltpu.SemaphoreType.DMA((8,)),
                pltpu.SemaphoreType.DMA((8,)),
                pltpu.SemaphoreType.DMA((8,)),
            ],
            compiler_params=pltpu.CompilerParams(
                collective_id=0, has_side_effects=True, vmem_limit_bytes=60 * 1024 * 1024),
        )(charge.reshape(1, slots), real_mask.reshape(1, slots), grid_idx.T, jnp.transpose(spline_w, (1, 2, 0)),
          influence, *[jnp.asarray(table) for table in tables])
        return mode_energy, energy[0, 0:1]

    return jax.shard_map(local_energy, mesh=mesh, in_specs=(slot_spec, slot_spec, P(('sys', 'ydom', 'zdom'), None), P(('sys', 'ydom', 'zdom'), None, None), mode_spec), out_specs=(mode_spec, P('sys')), check_vma=False)
```

```python
import functools
import math
import jax
import jax.numpy as jnp
import numpy as np
from jax import lax
from jax.experimental import pallas as pl
from jax.experimental.pallas import tpu as pltpu
from jax.sharding import PartitionSpec as P

MESH = pl.DeviceIdType.MESH
F32 = jnp.float32
BF16 = jnp.bfloat16
G = 96
Y_DEVS = 4
Z_DEVS = 2
LEN_Y = 24
LEN_Z = 48
KX = 24
KY = 48
STEP = 2048
SPLIT = 1
SECTIONS = 2
UNROLL = 6
PART = 1024
PREP = 512
ROWS = (368, 368, 368, 336)
BLOCKS = (12, 12, 12, 3, 4, 4, 4)
WIDTH = (384, 384, 384, 128, 128, 128, 128)
GHOSTS = 3
LAST = (4, 5, 6)
SLOT = (0, 12, 24, 12, 0, 4, 8)
EARLY = 36
LATE = 16


def split_np(values):
    high = np.asarray(values, np.float32).astype(jnp.bfloat16)
    low = (np.asarray(values, np.float64) - high.astype(np.float64)).astype(jnp.bfloat16)
    return high, low


def dft_x():
    table = np.zeros((Y_DEVS, 2, KX, 128))
    for dest in range(Y_DEVS):
        angle = 2 * math.pi * (np.outer(np.arange(KX) + KX * dest, np.arange(G)) % G) / G
        table[dest, 0, :, :G] = np.cos(angle)
        table[dest, 1, :, :G] = -np.sin(angle)
    high, low = split_np(table.reshape(Y_DEVS * 2 * KX, 128))
    return np.concatenate([high, high], axis=1), low


def dft_y():
    table = np.zeros((2, Y_DEVS, 32, Z_DEVS, 128))
    for source in range(Y_DEVS):
        y_pos = LEN_Y * source + np.arange(LEN_Y + 3)
        for dest in range(Z_DEVS):
            angle = 2 * math.pi * (np.outer(y_pos, np.arange(KY) + KY * dest) % G) / G
            table[0, source, :LEN_Y + 3, dest, :KY] = np.cos(angle)
            table[1, source, :LEN_Y + 3, dest, :KY] = np.sin(angle)
            table[0, source, :LEN_Y + 3, dest, KY:2 * KY] = -np.sin(angle)
            table[1, source, :LEN_Y + 3, dest, KY:2 * KY] = np.cos(angle)
    return split_np(table.reshape(2 * Y_DEVS * 32, Z_DEVS * 128))


def dft_z(messages, slots):
    table = np.zeros((Z_DEVS, slots, 2, 128))
    for source in range(Z_DEVS):
        for message in messages:
            for block in range(BLOCKS[message]):
                if message == GHOSTS:
                    z_pos = LEN_Z + block
                elif message in LAST:
                    z_pos = 4 * (4 * (message - LAST[0]) + block) + 3
                else:
                    z_pos = 4 * block + message
                angle = 2 * math.pi * (((z_pos + LEN_Z * source) * np.arange(G)) % G) / G
                table[source, SLOT[message] + block, 0, :G] = np.cos(angle)
                table[source, SLOT[message] + block, 1, :G] = np.sin(angle)
    return split_np(table.reshape(Z_DEVS * slots, 256))


def split(values):
    high = values.astype(BF16)
    return high, (values - high.astype(F32)).astype(BF16)


def dot(lhs, rhs, lhs_dim, rhs_dim):
    return lax.dot_general(lhs, rhs, (((lhs_dim,), (rhs_dim,)), ((), ())), preferred_element_type=F32)


def kernel(charge_in, mask_in, grid_idx_in, spline_w_in, influence_in, fx2_in, fx_low_in, fy_high_in, fy_low_in, early_high_in,
           early_low_in, late_in, mode, energy_out,
           charge, mask, grid_idx, spline_w, influence, fx2, fx_low, fy_high, fy_low, early_high, early_low, late,
           line_y, taps, base, lhs_a, lhs_b, rhs_a, rhs_b, total, packed, ghosts, *more):
    slots = charge_in.shape[1]
    me_y = lax.axis_index('ydom')
    me_z = lax.axis_index('zdom')
    me = me_z * Y_DEVS + me_y
    count = len(BLOCKS)
    sends, recvs, halves = more[:count], more[count:2 * count], more[2 * count:3 * count]
    (z_early, z_late, sums, part, parts,
     y_send_sem, y_recv_sem, z_send_sem, z_recv_sem, e_send_sem, e_recv_sem, in_sem, slot_sem) = more[3 * count:]

    def section(index):
        at = pl.ds(index * (slots // SECTIONS), slots // SECTIONS)
        return [pltpu.make_async_copy(source.at[..., at], dest.at[..., at], slot_sem.at[index, number])
                for number, (source, dest) in enumerate((
                    (charge_in, charge), (mask_in, mask), (grid_idx_in, grid_idx), (spline_w_in, spline_w)))]

    for index in range(SECTIONS):
        for load in section(index):
            load.start()
    loads = [pltpu.make_async_copy(source, dest, in_sem.at[index]) for index, (source, dest) in enumerate((
        (fx2_in, fx2), (fx_low_in, fx_low), (fy_high_in, fy_high), (fy_low_in, fy_low), (early_high_in, early_high),
        (early_low_in, early_low), (late_in, late), (influence_in, influence)))]
    for load in loads:
        load.start()

    def device(rank):
        return {'zdom': rank // Y_DEVS, 'ydom': rank % Y_DEVS}

    barrier = pltpu.get_barrier_semaphore()
    for shift in range(1, 8):
        pl.semaphore_signal(barrier, inc=1, device_id=device((me + shift) % 8), device_id_type=MESH)

    row4 = lax.broadcasted_iota(jnp.int32, (4, PREP), 0)
    row16 = lax.broadcasted_iota(jnp.int32, (16, PART), 0)
    row40 = lax.broadcasted_iota(jnp.int32, (40, PREP), 0)
    row40 = jnp.where(row40 < 32, row40, row40 % 4 + 24)
    row16_f = row16.astype(F32)

    def prepare(start):
        at = pl.ds(start, PREP)
        base_x, base_y, base_z = grid_idx[0:1, at], grid_idx[1:2, at], grid_idx[2:3, at]
        weight = charge[0:1, at] * mask[0:1, at].astype(F32)
        values = jnp.zeros((40, PREP), F32)
        for tap in range(4):
            values = jnp.where(row40 == base_y + tap, spline_w[1, tap:tap + 1, at], values)
        high = values.astype(BF16).astype(F32)
        for half, lines in ((0, high), (1, values - high)):
            for index, (top, bottom) in enumerate(((0, 1), (2, 0), (1, 2), (4, 4), (2, 3))):
                line_y[index, half, :, at] = jnp.concatenate(
                    [lines[8 * top:8 * top + 8], lines[8 * bottom:8 * bottom + 8]], axis=0).astype(BF16)
        tap = (row4 - base_z) & 3
        values = jnp.where(tap < 2, jnp.where(tap == 0, spline_w[2, 0:1, at], spline_w[2, 1:2, at]),
                           jnp.where(tap == 2, spline_w[2, 2:3, at], spline_w[2, 3:4, at]))
        block = ((base_z + tap) >> 2).astype(F32)
        base[:, at] = base_x.astype(F32)
        weight_x = spline_w[0, :, at] * weight
        for chunk in range(4):
            product = weight_x * values[chunk:chunk + 1]
            high = product.astype(BF16).astype(F32)
            taps[chunk, 0:4, at] = high
            taps[chunk, 4:8, at] = product - high
            taps[chunk, 8:9, at] = block[chunk:chunk + 1]

    def build(chunk, ghosts_too, start, to, lhs, rhs):
        at = pl.ds(start, PART)

        def spread_row(values):
            return jnp.broadcast_to(values, (16, PART)).astype(BF16)

        base_x = jnp.broadcast_to(base[:, at], (16, PART))
        rows = [spread_row(taps[chunk, index:index + 1, at]) for index in range(8)]
        zero = jnp.zeros((16, PART), BF16)
        offset = (row16_f - base_x).astype(BF16)
        wrapped = jnp.where(offset < jnp.asarray(-90, BF16), offset + jnp.asarray(G, BF16), offset)
        for group in range(G // 16):
            high, low = zero, zero
            for tap in range(4):
                hit = (offset if group else wrapped) == jnp.asarray(tap - 16 * group, BF16)
                high = jnp.where(hit, rows[tap], high)
                low = jnp.where(hit, rows[4 + tap], low)
            rhs[16 * group:16 * group + 16, to:to + PART] = high
            rhs[128 + 16 * group:144 + 16 * group, to:to + PART] = low
        block = jnp.broadcast_to(taps[chunk, 8:9, at], (16, PART))
        block_a = block.astype(BF16)
        block_b = (block - (row16 // 8).astype(F32)).astype(BF16)
        block_g = (block - (row16 // 4).astype(F32)).astype(BF16)
        tiles = []
        for pair in range(6):
            tiles += [(block_a, 2 * pair, 0), (block_b, 2 * pair, 1), (block_a, 2 * pair + 1, 2)]
        tiles += [(block_g, 0, 3), (block_g, 4, 3), (block_g, 8, 3)]
        if ghosts_too:
            tiles += [(block_a, 12, 0), (block_a, 12, 4)]
        for index, (source, value, pattern) in enumerate(tiles):
            hit = source == jnp.asarray(value, BF16)
            for half in range(2):
                lhs[half * ROWS[0] + 16 * index:half * ROWS[0] + 16 * index + 16, to:to + PART] = jnp.where(
                    hit, line_y[pattern, half, :, at], zero)

    def spread(chunk, first, last):
        rows = ROWS[chunk]

        count = slots // STEP

        def fill(step, lhs, rhs):
            ahead = step // count if chunk < 3 else 0
            start = pl.multiple_of((step % count) * STEP, STEP)
            for to in range(0, STEP, PART):
                build(chunk + ahead, chunk < 3, start + to, to, lhs, rhs)

        def add(lhs, rhs):
            product = dot(jnp.concatenate([lhs[0:rows, :], lhs[ROWS[0]:ROWS[0] + rows, :]], axis=0), rhs[...], 1, 1)
            total[0:rows, :] += product[:rows] + product[rows:]

        if first == 0:
            total[...] = jnp.zeros_like(total)
            if chunk == 0:
                fill(0, lhs_a, rhs_a)

        def body(pair, carry):
            add(lhs_a, rhs_a)
            fill(2 * pair + 1, lhs_b, rhs_b)
            add(lhs_b, rhs_b)
            fill(2 * pair + 2, lhs_a, rhs_a)
            return carry

        lax.fori_loop(first, last, body, 0)

    row8 = lax.broadcasted_iota(jnp.int32, (8, 128), 0)

    def pack(chunk, first, last):
        def lines(start, rows):
            return total[start:start + rows, 0:128] + total[start:start + rows, 128:256]

        for pair in range(first, last):
            ghost = lines(288 + 8 * pair, 8)
            packed[64 * pair:64 * pair + 24, :] = lines(48 * pair, 24)
            packed[64 * pair + 24:64 * pair + 32, :] = jnp.where(row8 < 4, ghost, 0.0)
            packed[64 * pair + 32:64 * pair + 56, :] = lines(48 * pair + 24, 24)
            packed[64 * pair + 56:64 * pair + 64, :] = jnp.where(row8 < 4, pltpu.roll(ghost, 4, 0), 0.0)
        if chunk < 3:
            ghosts[32 * chunk:32 * chunk + 32, :] = lines(336, 32)

    def transform_x(message, values):
        high, low = split(values)
        lines_k = dot(fx2[...], jnp.concatenate([high, low], axis=1), 1, 1) + dot(fx_low[...], high, 1, 1)
        for dest in range(Y_DEVS):
            sends[message][dest] = lines_k[48 * dest:48 * dest + 48]
        recvs[message][me_y] = sends[message][me_y]

    def copy_y(chunk, shift):
        dest = (me_y + shift) % Y_DEVS
        return pltpu.make_async_remote_copy(
            src_ref=sends[chunk].at[dest], dst_ref=recvs[chunk].at[me_y],
            send_sem=y_send_sem.at[chunk, shift], recv_sem=y_recv_sem.at[chunk, shift],
            device_id={'ydom': dest}, device_id_type=MESH)

    def start_y(chunk):
        for shift in (2, 1, 3):
            copy_y(chunk, shift).start()

    def wait_y(chunk):
        for shift in (2, 1, 3):
            copy_y(chunk, shift).wait()

    lane = lax.broadcasted_iota(jnp.int32, (KX, 128), 1)

    def regroup(blocks):
        out = list(blocks)
        for first, second in ((0, 2), (1, 3)):
            one, two = out[first], out[second]
            out[first] = jnp.where(lane < 64, one, pltpu.roll(two, 64, 1))
            out[second] = jnp.where(lane < 64, pltpu.roll(one, 64, 1), two)
        for first, second in ((0, 1), (2, 3)):
            one, two = out[first], out[second]
            even = (lane // 32) % 2 == 0
            out[first] = jnp.where(even, one, pltpu.roll(two, 32, 1))
            out[second] = jnp.where(even, pltpu.roll(one, 96, 1), two)
        return out

    def z_rows(message):
        per_source = EARLY if message < GHOSTS else LATE
        return pl.ds((me_z * per_source + SLOT[message]) * KX, BLOCKS[message] * KX)

    def z_buffer(message):
        return z_early if message < GHOSTS else z_late

    def copy_z(message):
        return pltpu.make_async_remote_copy(
            src_ref=halves[message], dst_ref=z_buffer(message).at[z_rows(message)],
            send_sem=z_send_sem.at[message], recv_sem=z_recv_sem.at[message],
            device_id={'zdom': 1 - me_z}, device_id_type=MESH)

    def transform_y(message):
        recv = recvs[message]
        lines_re, lines_im = [], []
        for tile in range(WIDTH[message] // 128):
            for part_id, lines in ((0, lines_re), (1, lines_im)):
                lines += regroup([recv[source, KX * part_id:KX * part_id + KX, 128 * tile:128 * tile + 128]
                                  for source in range(Y_DEVS)])
        blocks = BLOCKS[message]
        values = jnp.concatenate([jnp.concatenate(lines_re[:blocks], axis=0), jnp.concatenate(lines_im[:blocks], axis=0)], axis=1)
        high, low = split(values)
        lines_k = dot(high, fy_high[...], 1, 0) + dot(high, fy_low[...], 1, 0) + dot(low, fy_high[...], 1, 0)
        first = me_z == 0
        halves[message][...] = jnp.where(first, lines_k[:, 128:], lines_k[:, :128])
        z_buffer(message)[z_rows(message), :] = jnp.where(first, lines_k[:, :128], lines_k[:, 128:])

    for rhs in (rhs_a, rhs_b):
        for row in (G, 128 + G):
            rhs[row:row + 32, :] = jnp.zeros((32, STEP), BF16)
    ghosts[...] = jnp.zeros_like(ghosts)
    for source in range(Z_DEVS):
        z_late[((source + 1) * LATE - 1) * KX:(source + 1) * LATE * KX, :] = jnp.zeros((KX, 128), F32)

    def prepare_step(step, carry):
        prepare(pl.multiple_of(step * PREP, PREP))
        return carry

    part_steps = slots // PREP // SECTIONS
    for index in range(SECTIONS):
        for load in section(index):
            load.wait()
        lax.fori_loop(index * part_steps, (index + 1) * part_steps, prepare_step, 0)

    steps = slots // STEP // 2
    for chunk in range(3):
        spread(chunk, 0, steps)
        if chunk == 0:
            for load in loads:
                load.wait()
            pl.semaphore_wait(barrier, 7)
        else:
            wait_y(chunk - 1)
        pack(chunk, 0, 6)
        transform_x(chunk, packed[...])
        if chunk == 2:
            transform_x(GHOSTS, ghosts[...])
        if chunk > 0:
            transform_y(chunk - 1)
        start_y(chunk)
        if chunk == 2:
            start_y(GHOSTS)
        if chunk > 0:
            copy_z(chunk - 1).start()
    spread(3, 0, steps - SPLIT)
    wait_y(2)
    transform_y(2)
    copy_z(2).start()
    spread(3, steps - SPLIT, steps)
    for index, message in enumerate(LAST):
        pack(3, 2 * index, 2 * index + 2)
        transform_x(message, packed[128 * index:128 * index + 128, :])
        start_y(message)
    wait_y(GHOSTS)
    transform_y(GHOSTS)
    copy_z(GHOSTS).start()
    def sum_early(index, carry):
        high, low = split(z_early[pl.ds(index, Z_DEVS * EARLY, stride=KX), :])
        high, low = high[:, :2 * KY], low[:, :2 * KY]
        sums[index] = dot(high, early_high[...], 0, 0) + dot(high, early_low[...], 0, 0) + dot(low, early_high[...], 0, 0)
        return carry

    for index, message in enumerate(LAST):
        wait_y(message)
        transform_y(message)
        copy_z(message).start()
        if index == 0:
            for early in range(3):
                copy_z(early).wait()
            lax.fori_loop(0, KX // 2, sum_early, 0, unroll=UNROLL)
        elif index == 1:
            lax.fori_loop(KX // 2, KX, sum_early, 0, unroll=UNROLL)
    for message in (GHOSTS,) + LAST:
        copy_z(message).wait()

    def sum_late(index, energy_sum):
        high, low = split(z_late[pl.ds(index, Z_DEVS * LATE, stride=KX), :])
        values = jnp.concatenate([high, low, high], axis=0)[:, :2 * KY]
        lines_k = sums[index] + dot(values, late[...], 0, 0)
        real = lines_k[0:KY, 0:G] + lines_k[KY:2 * KY, 128:128 + G]
        imag = lines_k[KY:2 * KY, 0:G] - lines_k[0:KY, 128:128 + G]
        energy = 0.5 * influence[index] * (real * real + imag * imag)
        mode[index] = energy
        return energy_sum + energy

    energy_sum = jnp.zeros((KY, G), F32)
    for index in range(3):
        energy_sum = lax.fori_loop(8 * index, 8 * index + 8, sum_late, energy_sum, unroll=8)
    part[...] = jnp.broadcast_to(jnp.sum(energy_sum), (8, 128))
    parts[me] = part[...]

    def copy_e(shift):
        return pltpu.make_async_remote_copy(
            src_ref=part, dst_ref=parts.at[me], send_sem=e_send_sem.at[shift], recv_sem=e_recv_sem.at[shift],
            device_id=device((me + shift) % 8), device_id_type=MESH)

    for shift in range(1, 8):
        copy_e(shift).start()
    for shift in range(1, 8):
        copy_e(shift).wait()
    result = parts[0]
    for rank in range(1, 8):
        result = result + parts[rank]
    energy_out[...] = result * (1.0 / (G * G * G))


def solution(mesh):
    slot_spec = P(('sys', 'ydom', 'zdom'))
    mode_spec = P(('sys', 'ydom'), 'zdom', None)
    late_high, late_low = dft_z((GHOSTS,) + LAST, LATE)
    tables = dft_x() + dft_y() + dft_z((0, 1, 2), EARLY) + (np.concatenate([late_high, late_high, late_low], axis=0),)

    def local_energy(charge, real_mask, grid_idx, spline_w, influence):
        slots = charge.shape[0]
        vmem = pl.BlockSpec(memory_space=pltpu.VMEM)
        whole = pl.BlockSpec(memory_space=pl.ANY)
        mode_energy, energy = pl.pallas_call(
            kernel,
            out_shape=(pltpu.VMEM((KX, KY, G), F32), pltpu.VMEM((8, 128), F32)),
            in_specs=[whole] * (5 + len(tables)),
            out_specs=(vmem, vmem),
            scratch_shapes=[
                pltpu.VMEM((1, slots), F32),
                pltpu.VMEM((1, slots), jnp.int32),
                pltpu.VMEM((3, slots), jnp.int32),
                pltpu.VMEM((3, 4, slots), F32),
                pltpu.VMEM(influence.shape, F32),
            ] + [pltpu.VMEM(table.shape, BF16) for table in tables] + [
                pltpu.VMEM((5, 2, 16, slots), BF16),
                pltpu.VMEM((4, 9, slots), F32),
                pltpu.VMEM((1, slots), F32),
                pltpu.VMEM((2 * ROWS[0], STEP), BF16),
                pltpu.VMEM((2 * ROWS[0], STEP), BF16),
                pltpu.VMEM((256, STEP), BF16),
                pltpu.VMEM((256, STEP), BF16),
                pltpu.VMEM((ROWS[0], 256), F32),
                pltpu.VMEM((384, 128), F32),
                pltpu.VMEM((128, 128), F32),
            ] + [pltpu.VMEM((Y_DEVS, 2 * KX, width), F32) for width in WIDTH] * 2
            + [pltpu.VMEM((blocks * KX, 128), F32) for blocks in BLOCKS] + [
                pltpu.VMEM((Z_DEVS * EARLY * KX, 128), F32),
                pltpu.VMEM((Z_DEVS * LATE * KX, 128), F32),
                pltpu.VMEM((KX, 2 * KY, 256), F32),
                pltpu.VMEM((8, 128), F32),
                pltpu.VMEM((8, 8, 128), F32),
                pltpu.SemaphoreType.DMA((len(BLOCKS), 4)),
                pltpu.SemaphoreType.DMA((len(BLOCKS), 4)),
                pltpu.SemaphoreType.DMA((len(BLOCKS),)),
                pltpu.SemaphoreType.DMA((len(BLOCKS),)),
                pltpu.SemaphoreType.DMA((8,)),
                pltpu.SemaphoreType.DMA((8,)),
                pltpu.SemaphoreType.DMA((8,)),
                pltpu.SemaphoreType.DMA((SECTIONS, 4)),
            ],
            compiler_params=pltpu.CompilerParams(
                collective_id=0, has_side_effects=True, vmem_limit_bytes=60 * 1024 * 1024),
        )(charge.reshape(1, slots), real_mask.reshape(1, slots), grid_idx.T, jnp.transpose(spline_w, (1, 2, 0)),
          influence, *[jnp.asarray(table) for table in tables])
        return mode_energy, energy[0, 0:1]

    return jax.shard_map(local_energy, mesh=mesh, in_specs=(slot_spec, slot_spec, P(('sys', 'ydom', 'zdom'), None), P(('sys', 'ydom', 'zdom'), None, None), mode_spec), out_specs=(mode_spec, P('sys')), check_vma=False)
```
